256 devices in a mesh: grp: 32 (over z, x_lo, core), tile: 8 (over x_hi, y).
Axes of the slice: x: 4 (x_hi: 2, x_lo: 2; x = x_hi * 2 + x_lo), y: 4, z: 8, core: 2. Of those that a mesh axis runs over, the one named last changes fastest.
Arguments:
- spectrum: float32 [1152, 256, 512], P(None, 'tile', 'grp'), may hold values from 0.05 to 2
- matrices: bfloat16 [8, 32, 2, 1152, 1152], P('tile', 'grp'), may hold values from -0.1875 to 0.1875
- ownership: int32 [256, 512], P('tile', 'grp'), may hold values from 0 to 1
- land_mask: int32 [256, 512], P('tile', 'grp'), may hold values 0 or 1
- courant: float32 [2, 1152], replicated, may hold values from -0.45 to 0.45
- stokes_weight: bfloat16 [1152, 256], replicated, may hold values from -0.1875 to 0.1875
- ocean: float32 [4, 256, 512, 128], P(None, 'tile', 'grp'), may hold values from -6 to 6
Outputs:
- spectrum_out: float32 [1152, 256, 512], P(None, 'tile', 'grp')
- ocean_out: float32 [4, 256, 512, 128], P(None, 'tile', 'grp')
The draws below stay inside these ranges and needn't reach their ends.
All inputs are finite; a program needn't handle non-finite values. No bound on the sum of `land_mask` on one device may be relied on, other than what follows from the above.
Results may differ from the reference program's by a relative error of at most 0.0021.
Values sent between devices are 32-bit elements; how exact they have to be, the bound alone decides.
A program may use at most 128 MiB of HBM per device.

```python
import math
import jax
import jax.numpy as jnp
from jax import lax

BINS = 1152
LEVELS = 128
MATS = 2
STEPS = 2
ROWS_DEV = 32
COLS_DEV = 16
NR = 256
NC = 512
N_GRP = 32
N_TILE = 8


def plant(values, key, least, top_value):
    longest = values.shape.index(max(values.shape))
    spots = []
    for shift in (0, 1):
        where = [jax.random.randint(jax.random.fold_in(key, axis), (), 0, length) for axis, length in enumerate(values.shape)]
        where[longest] = (where[longest] + shift) % values.shape[longest]
        spots.append(tuple(where))
    return values.at[spots[0]].set(least).at[spots[1]].set(top_value)


def block_levels(key, shape, shards, low, top_value):
    def one(position, parts):
        draws = jax.random.uniform(jax.random.fold_in(jax.random.fold_in(key, 6), position), (parts,), jnp.float32, low / len(shards), top_value / len(shards))
        return jnp.repeat(jnp.exp(draws), shape[position] // parts).reshape((-1,) + (1,) * (len(shape) - position - 1))

    level = one(*shards[0])
    for cut in shards[1:]:
        level = level * one(*cut)
    return level


def bell_draw(rng, extent, spread, bound, cuts=(), held_as=jnp.bfloat16):
    result = spread * jax.random.normal(rng, extent, jnp.float32)
    if cuts:
        result = result * block_levels(rng, extent, cuts, -0.22, 0.18)
    return jnp.clip(result, -bound, bound).astype(held_as)


def setup_inputs(seed: int = 0) -> dict:
    splits = jax.random.split(jax.random.key(seed), 8)
    return {
        "spectrum": jnp.clip(jnp.exp(math.log(2.0) - 3.6888794 * jax.random.uniform(splits[0], (BINS, NR, NC), jnp.float32) ** block_levels(splits[0], (BINS, NR, NC), ((1, 8), (2, 32)), -0.2, 0.2)), 0.05, 2.0),
        "matrices": bell_draw(splits[1], (N_TILE, N_GRP, MATS, BINS, BINS), BINS ** -0.5, 0.1875, ((0, 8), (1, 32))),
        "ownership": plant(jax.random.randint(splits[2], (NR, NC), 0, MATS), jax.random.fold_in(splits[2], 1), 0, MATS - 1).astype(jnp.int32),
        "land_mask": plant((jax.random.randint(splits[3], (NR, NC), 0, 10) < 9).astype(jnp.int32), jax.random.fold_in(splits[3], 1), 0, 1),
        "courant": jnp.clip(jax.random.uniform(splits[4], (2, BINS), jnp.float32, -0.45, 0.45), -0.45, 0.45),
        "stokes_weight": bell_draw(splits[5], (BINS, 2 * LEVELS), BINS ** -0.5, 0.1875),
        "ocean": bell_draw(splits[6], (4, NR, NC, LEVELS), 1.0, 6.0, ((1, 8), (2, 32)), jnp.float32),
    }


current_gain = 0.2
source_gain = 0.5
mixing_side = 0.15
mixing_depth = 0.2
rotation = 0.3
transport = 0.5


def upwind(padded, speed_x, speed_y, sea_mask):
    middle = padded[:, 1:-1, 1:-1]
    western = padded[:, 1:-1, :-2]
    eastern = padded[:, 1:-1, 2:]
    northern = padded[:, :-2, 1:-1]
    southern = padded[:, 2:, 1:-1]
    flux = jnp.maximum(speed_x, 0.0) * (middle - western) + jnp.minimum(speed_x, 0.0) * (eastern - middle)
    flux = flux + jnp.maximum(speed_y, 0.0) * (middle - northern) + jnp.minimum(speed_y, 0.0) * (southern - middle)
    return sea_mask[None] * (middle - flux)


def ocean_step(fields, padded, drift, sea_mask):
    northern = padded[:, :-2, 1:-1]
    southern = padded[:, 2:, 1:-1]
    western = padded[:, 1:-1, :-2]
    eastern = padded[:, 1:-1, 2:]
    lateral = northern + southern + western + eastern - 4.0 * fields
    column = jnp.pad(fields, ((0, 0), (0, 0), (0, 0), (1, 1)))
    vertical = column[..., 2:] + column[..., :-2] - 2.0 * fields
    mixing = mixing_side * lateral + mixing_depth * vertical
    tend_u = mixing[0] + rotation * (fields[1] + drift[1])
    tend_v = mixing[1] - rotation * (fields[0] + drift[0])
    grad_x = 0.5 * (eastern[2:] - western[2:])
    grad_y = 0.5 * (southern[2:] - northern[2:])
    tend_tracer = mixing[2:] - transport * (drift[0][None] * grad_x + drift[1][None] * grad_y)
    tendency = jnp.concatenate([tend_u[None], tend_v[None], tend_tracer], 0)
    return fields + sea_mask[None, :, :, None] * tendency


def reference(spectrum, matrices, ownership, land_mask, courant, stokes_weight, ocean):
    sea_mask = land_mask.astype(jnp.float32)
    blocks_count = N_TILE * N_GRP
    points = ROWS_DEV * COLS_DEV
    matrix_set = matrices.reshape(blocks_count, MATS, BINS, BINS)
    owner_blocks = ownership.reshape(N_TILE, ROWS_DEV, N_GRP, COLS_DEV).transpose(0, 2, 1, 3).reshape(blocks_count, 1, 1, points)
    choices_range = jnp.arange(MATS, dtype=jnp.int32)[:, None, None]
    profile = stokes_weight.astype(jnp.float32).reshape(BINS, 2, LEVELS)
    energy = spectrum
    fields = ocean
    for step in range(STEPS):
        current = fields[0:2, :, :, 0]
        speed_x = courant[0][:, None, None] + current_gain * current[0][None]
        speed_y = courant[1][:, None, None] + current_gain * current[1][None]
        padded = jnp.pad(energy, ((0, 0), (1, 1), (1, 1)))
        advected = upwind(padded, speed_x, speed_y, sea_mask)
        low = advected.astype(jnp.bfloat16)
        low_blocks = low.reshape(BINS, N_TILE, ROWS_DEV, N_GRP, COLS_DEV).transpose(1, 3, 0, 2, 4).reshape(blocks_count, BINS, points)

        def apply_block(items):
            matrix_pair, block, owner = items
            products = jnp.einsum("mab,bp->map", matrix_pair.astype(jnp.float32), block.astype(jnp.float32))
            select = (owner[0] == choices_range).astype(jnp.float32)
            return jnp.sum(select * products, axis=0)

        source_blocks = lax.map(apply_block, (matrix_set, low_blocks, owner_blocks))
        source = source_blocks.reshape(N_TILE, N_GRP, BINS, ROWS_DEV, COLS_DEV).transpose(2, 0, 3, 1, 4).reshape(BINS, NR, NC)
        energy = sea_mask[None] * (advected + source_gain * source)
        drift = jnp.einsum("brc,bkl->krcl", energy.astype(jnp.bfloat16).astype(jnp.float32), profile)
        padded_ocean = jnp.pad(fields, ((0, 0), (1, 1), (1, 1), (0, 0)))
        fields = ocean_step(fields, padded_ocean, drift, sea_mask)
    return energy, fields
```

```python
import functools
import jax
import jax.numpy as jnp
from jax import lax
from jax.sharding import PartitionSpec as P
from jax.experimental import pallas as pl
from jax.experimental.pallas import tpu as pltpu

STEPS = 2
current_gain = 0.2
source_gain = 0.5
mixing_side = 0.15
mixing_depth = 0.2
rotation = 0.3
transport = 0.5

LANES = 128
PITCH = 24
LEAD = 8
W, E, N, S = range(4)


def kernel(rows, cols, tiles, mats_count,
           e0, mats, own_h, mask_h, cour_h, stok_h, oc,
           e_out, o_out,
           ebuf, xbuf, low, elow, mbuf, stok, cour, ownv, maskv, obuf,
           sea, o0, o1, ux, uy, drift,
           epack, ehx, ehy, opack, ohx, ohy,
           lsem, esem, ersem, osem, orsem, wsem):
    g = lax.axis_index("grp")
    t = lax.axis_index("tile")
    ng = lax.axis_size("grp")
    nt = lax.axis_size("tile")
    bins = tiles * LANES
    points = rows * cols
    has = [g > 0, g < ng - 1, t > 0, t < nt - 1]
    peer = [{"grp": g - 1}, {"grp": g + 1}, {"tile": t - 1}, {"tile": t + 1}]
    back = [E, W, S, N]
    chunks = [(k, min(2, tiles - k)) for k in range(0, tiles, 2)]
    fields = obuf.shape[1]

    e4 = ebuf.reshape(tiles, rows + 2, PITCH, LANES)
    o5 = obuf.reshape(2, fields, rows + 2, PITCH, LANES)

    loads = []

    def load(src, dst):
        copy = pltpu.make_async_copy(src, dst, lsem.at[len(loads)])
        copy.start()
        loads.append(copy)
        return copy

    e_load = [load(e0.at[:, :, pl.ds(k * LANES, LANES)], e4.at[k, pl.ds(1, rows), pl.ds(LEAD, cols), :]) for k in range(tiles)]
    small = [load(oc, o5.at[0, :, pl.ds(1, rows), pl.ds(LEAD, cols), :]),
             load(cour_h, cour), load(mask_h, maskv), load(own_h, ownv)]
    m_load = []
    for k, width in chunks:
        span = pl.ds(k * LANES, width * LANES)
        m_load.append([load(mats.at[m, span, :], mbuf.at[span, pl.ds(m * bins, bins)]) for m in range(mats_count)])
    stok_load = load(stok_h, stok)

    barrier = pltpu.get_barrier_semaphore()
    for d in range(4):
        @pl.when(has[d])
        def _(d=d):
            pl.semaphore_signal(barrier, inc=1, device_id=peer[d], device_id_type=pl.DeviceIdType.MESH)

    for d in range(4):
        @pl.when(jnp.logical_not(has[d]))
        def _(d=d):
            if d < 2:
                ehx[:, d] = jnp.zeros_like(ehx[:, d])
                ohx[:, d] = jnp.zeros_like(ohx[:, d])
            else:
                ehy[:, d - 2] = jnp.zeros_like(ehy[:, d - 2])
                ohy[:, d - 2] = jnp.zeros_like(ohy[:, d - 2])

    def e_copy(step, d, c):
        k, width = chunks[c]
        span = pl.ds(k, width)
        far = back[d]
        if d < 2:
            src = epack.at[step, d, span]
            dst = ehx.at[step, far, span]
        else:
            src = e4.at[span, 1 if d == N else rows, pl.ds(LEAD, cols), :]
            dst = ehy.at[step, far - 2, span]
        return pltpu.make_async_remote_copy(
            src_ref=src, dst_ref=dst, send_sem=esem.at[step, d, c], recv_sem=ersem.at[step, far, c],
            device_id=peer[d], device_id_type=pl.DeviceIdType.MESH)

    def e_arrival(step, side, c):
        k, width = chunks[c]
        span = pl.ds(k, width)
        dst = ehx.at[step, side, span] if side < 2 else ehy.at[step, side - 2, span]
        return pltpu.make_async_remote_copy(
            src_ref=dst, dst_ref=dst, send_sem=esem.at[step, side, c], recv_sem=ersem.at[step, side, c],
            device_id=peer[side], device_id_type=pl.DeviceIdType.MESH)

    def o_copy(step, d):
        far = back[d]
        if d < 2:
            src = opack.at[step, d]
            dst = ohx.at[step, far]
        else:
            src = o5.at[step, :, 1 if d == N else rows, pl.ds(LEAD, cols), :]
            dst = ohy.at[step, far - 2]
        return pltpu.make_async_remote_copy(
            src_ref=src, dst_ref=dst, send_sem=osem.at[step, d], recv_sem=orsem.at[step, far],
            device_id=peer[d], device_id_type=pl.DeviceIdType.MESH)

    def o_arrival(step, side):
        dst = ohx.at[step, side] if side < 2 else ohy.at[step, side - 2]
        return pltpu.make_async_remote_copy(
            src_ref=dst, dst_ref=dst, send_sem=osem.at[step, side], recv_sem=orsem.at[step, side],
            device_id=peer[side], device_id_type=pl.DeviceIdType.MESH)

    first_col = pl.ds(PITCH + LEAD, rows, stride=PITCH)
    last_col = pl.ds(PITCH + LEAD + cols - 1, rows, stride=PITCH)
    west_col = pl.ds(PITCH + LEAD - 1, rows, stride=PITCH)
    east_col = pl.ds(PITCH + LEAD + cols, rows, stride=PITCH)

    def e_pack(step, c):
        k0, width = chunks[c]
        for k in range(k0, k0 + width):
            epack[step, W, k] = ebuf[k, first_col, :]
            epack[step, E, k] = ebuf[k, last_col, :]

    def o_pack(step):
        for q in range(fields):
            opack[step, W, q] = obuf[step, q, first_col, :]
            opack[step, E, q] = obuf[step, q, last_col, :]

    def send(make):
        for d in range(4):
            @pl.when(has[d])
            def _(d=d):
                make(d).start()

    def wait_recv(make):
        for d in range(4):
            @pl.when(has[d])
            def _(d=d):
                make(d).wait_recv()

    def wait_send(make):
        for d in range(4):
            @pl.when(has[d])
            def _(d=d):
                make(d).wait_send()

    for c, (k0, width) in enumerate(chunks):
        for k in range(k0, k0 + width):
            e_load[k].wait()
        e_pack(0, c)
        if c == 0:
            pl.semaphore_wait(barrier, sum(h.astype(jnp.int32) for h in has))
        send(lambda d: e_copy(0, d, c))
    for copy in small:
        copy.wait()
    o_pack(0)
    send(lambda d: o_copy(0, d))

    mask_all = maskv[...].astype(jnp.float32)
    own_all = ownv[...]
    own0 = jnp.where(own_all == 0, 1.0, 0.0)
    own1 = jnp.where(own_all == 1, 1.0, 0.0)
    for r in range(rows):
        at = pl.ds(r * cols, cols)
        sea[at, :] = jnp.broadcast_to(mask_all[:, r:r + 1], (cols, LANES))
        o0[at, :] = jnp.broadcast_to(own0[:, r:r + 1], (cols, LANES))
        o1[at, :] = jnp.broadcast_to(own1[:, r:r + 1], (cols, LANES))
        for q, dst in ((0, ux), (1, uy)):
            here = obuf[0, q, pl.ds((r + 1) * PITCH + LEAD, cols), :]
            dst[at, :] = current_gain * jnp.broadcast_to(here[:, 0:1], (cols, LANES))

    def advect(step, k):
        cx = jnp.broadcast_to(cour[0:1, k * LANES:(k + 1) * LANES], (cols, LANES))
        cy = jnp.broadcast_to(cour[1:2, k * LANES:(k + 1) * LANES], (cols, LANES))

        @pl.loop(0, rows // 8)
        def _(block):
            for i in range(8):
                r = block * 8 + i
                base = (r + 1) * PITCH + LEAD
                at = pl.ds(pl.multiple_of(r * cols, cols), cols)
                mid = ebuf[k, pl.ds(base, cols), :]
                west = ebuf[k, pl.ds(base - 1, cols), :]
                east = ebuf[k, pl.ds(base + 1, cols), :]
                north = ebuf[k, pl.ds(base - PITCH, cols), :]
                south = ebuf[k, pl.ds(base + PITCH, cols), :]
                sx = cx + ux[at, :]
                sy = cy + uy[at, :]
                flux = sx * jnp.where(sx > 0.0, mid - west, east - mid)
                flux = flux + sy * jnp.where(sy > 0.0, mid - north, south - mid)
                adv = sea[at, :] * (mid - flux)
                xbuf[k, at, :] = adv
                low[at, k * LANES:(k + 1) * LANES] = (adv * o0[at, :]).astype(jnp.bfloat16)
                low[at, bins + k * LANES:bins + (k + 1) * LANES] = (adv * o1[at, :]).astype(jnp.bfloat16)

    lane = lax.broadcasted_iota(jnp.int32, (cols, LANES), 1)

    def ocean(step):
        dst_o = 1 - step

        @pl.loop(0, rows)
        def _(r):
            base = (r + 1) * PITCH + LEAD
            at = pl.ds(pl.multiple_of(r * cols, cols), cols)
            d0 = drift[at, 0:LANES]
            d1 = drift[at, LANES:2 * LANES]
            sm = sea[at, :]
            mids = [obuf[step, q, pl.ds(base, cols), :] for q in range(fields)]
            for q in range(fields):
                mid = mids[q]
                west = obuf[step, q, pl.ds(base - 1, cols), :]
                east = obuf[step, q, pl.ds(base + 1, cols), :]
                north = obuf[step, q, pl.ds(base - PITCH, cols), :]
                south = obuf[step, q, pl.ds(base + PITCH, cols), :]
                above = jnp.where(lane == LANES - 1, 0.0, pltpu.roll(mid, LANES - 1, 1))
                below = jnp.where(lane == 0, 0.0, pltpu.roll(mid, 1, 1))
                mix = mixing_side * (north + south + west + east - 4.0 * mid) + mixing_depth * (above + below - 2.0 * mid)
                if q == 0:
                    tend = mix + rotation * (mids[1] + d1)
                elif q == 1:
                    tend = mix - rotation * (mids[0] + d0)
                else:
                    tend = mix - transport * (d0 * (0.5 * (east - west)) + d1 * (0.5 * (south - north)))
                new = mid + sm * tend
                obuf[dst_o, q, pl.ds(base, cols), :] = new
                if step == 0 and q < 2:
                    dst = (ux, uy)[q]
                    dst[at, :] = current_gain * jnp.broadcast_to(new[:, 0:1], (cols, LANES))

    out_copies = []
    for step in range(STEPS):
        for c, (k0, width) in enumerate(chunks):
            wait_recv(lambda d: e_arrival(step, d, c))
            for k in range(k0, k0 + width):
                ebuf[k, west_col, :] = ehx[step, W, k]
                ebuf[k, east_col, :] = ehx[step, E, k]
                ebuf[k, pl.ds(LEAD, cols), :] = ehy[step, 0, k]
                ebuf[k, pl.ds((rows + 1) * PITCH + LEAD, cols), :] = ehy[step, 1, k]
                advect(step, k)
        for c in range(len(chunks)):
            wait_send(lambda d: e_copy(step, d, c))
        for c, (k0, width) in enumerate(chunks):
            if step == 0:
                for copy in m_load[c]:
                    copy.wait()
            src = lax.dot_general(
                low[...], mbuf[k0 * LANES:(k0 + width) * LANES, :], (((1,), (1,)), ((), ())),
                preferred_element_type=jnp.float32)
            for k in range(k0, k0 + width):
                part = src[:, (k - k0) * LANES:(k - k0 + 1) * LANES]
                new = sea[...] * (xbuf[k] + source_gain * part)
                e4[k, 1:rows + 1, LEAD:LEAD + cols, :] = new.reshape(rows, cols, LANES)
                elow[:, k * LANES:(k + 1) * LANES] = new.astype(jnp.bfloat16)
            if step + 1 < STEPS:
                e_pack(step + 1, c)
                send(lambda d: e_copy(step + 1, d, c))
            else:
                for k in range(k0, k0 + width):
                    copy = pltpu.make_async_copy(
                        e4.at[k, pl.ds(1, rows), pl.ds(LEAD, cols), :], e_out.at[:, :, pl.ds(k * LANES, LANES)], wsem.at[k])
                    copy.start()
                    out_copies.append(copy)
        if step == 0:
            stok_load.wait()
        drift[...] = jnp.dot(elow[...], stok[...], preferred_element_type=jnp.float32)
        wait_recv(lambda d: o_arrival(step, d))
        for q in range(fields):
            obuf[step, q, west_col, :] = ohx[step, W, q]
            obuf[step, q, east_col, :] = ohx[step, E, q]
            obuf[step, q, pl.ds(LEAD, cols), :] = ohy[step, 0, q]
            obuf[step, q, pl.ds((rows + 1) * PITCH + LEAD, cols), :] = ohy[step, 1, q]
        if step == 1:
            wait_send(lambda d: o_copy(0, d))
        ocean(step)
        if step + 1 < STEPS:
            o_pack(step + 1)
            send(lambda d: o_copy(step + 1, d))
    copy = pltpu.make_async_copy(
        o5.at[0, :, pl.ds(1, rows), pl.ds(LEAD, cols), :], o_out, wsem.at[tiles])
    copy.start()
    out_copies.append(copy)
    wait_send(lambda d: o_copy(1, d))
    for copy in out_copies:
        copy.wait()


def local(spectrum, matrices, ownership, land_mask, courant, stokes_weight, ocean):
    bins, rows, cols = spectrum.shape
    mats = matrices.reshape(matrices.shape[2:])
    count = mats.shape[0]
    tiles = bins // LANES
    points = rows * cols
    fields = ocean.shape[0]
    chunk_count = -(-tiles // 2)
    flat = (rows + 2) * PITCH
    e0 = jnp.transpose(spectrum, (1, 2, 0))
    f32 = jnp.float32
    any_spec = pl.BlockSpec(memory_space=pltpu.HBM)
    e_new, o_new = pl.pallas_call(
        functools.partial(kernel, rows, cols, tiles, count),
        out_shape=(jax.ShapeDtypeStruct((rows, cols, bins), f32), jax.ShapeDtypeStruct(ocean.shape, f32)),
        in_specs=[any_spec] * 7,
        out_specs=(any_spec, any_spec),
        scratch_shapes=[
            pltpu.VMEM((tiles, flat, LANES), f32),
            pltpu.VMEM((tiles, points, LANES), f32),
            pltpu.VMEM((points, count * bins), jnp.bfloat16),
            pltpu.VMEM((points, bins), jnp.bfloat16),
            pltpu.VMEM((bins, count * bins), jnp.bfloat16),
            pltpu.VMEM((bins, 2 * LANES), jnp.bfloat16),
            pltpu.VMEM((2, bins), f32),
            pltpu.VMEM((cols, rows), jnp.int32),
            pltpu.VMEM((cols, rows), jnp.int32),
            pltpu.VMEM((2, fields, flat, LANES), f32),
        ] + [pltpu.VMEM((points, LANES), f32)] * 5 + [
            pltpu.VMEM((points, 2 * LANES), f32),
            pltpu.VMEM((STEPS, 2, tiles, rows, LANES), f32),
            pltpu.VMEM((STEPS, 2, tiles, rows, LANES), f32),
            pltpu.VMEM((STEPS, 2, tiles, cols, LANES), f32),
            pltpu.VMEM((STEPS, 2, fields, rows, LANES), f32),
            pltpu.VMEM((STEPS, 2, fields, rows, LANES), f32),
            pltpu.VMEM((STEPS, 2, fields, cols, LANES), f32),
            pltpu.SemaphoreType.DMA((tiles + 5 + chunk_count * count,)),
            pltpu.SemaphoreType.DMA((STEPS, 4, chunk_count)),
            pltpu.SemaphoreType.DMA((STEPS, 4, chunk_count)),
            pltpu.SemaphoreType.DMA((STEPS, 4)),
            pltpu.SemaphoreType.DMA((STEPS, 4)),
            pltpu.SemaphoreType.DMA((tiles + 1,)),
        ],
        compiler_params=pltpu.CompilerParams(
            collective_id=0, has_side_effects=True, vmem_limit_bytes=56 * 1024 * 1024),
    )(e0, mats, ownership.T, land_mask.T, courant, stokes_weight, ocean)
    return jnp.transpose(e_new, (2, 0, 1)), o_new


def solution(mesh):
    in_specs = (
        P(None, "tile", "grp"),
        P("tile", "grp", None, None, None),
        P("tile", "grp"),
        P("tile", "grp"),
        P(),
        P(),
        P(None, "tile", "grp", None),
    )
    out_specs = (P(None, "tile", "grp"), P(None, "tile", "grp", None))
    return jax.shard_map(local, mesh=mesh, in_specs=in_specs, out_specs=out_specs, check_vma=False)
```

```python
import functools
import jax
import jax.numpy as jnp
from jax import lax
from jax.sharding import PartitionSpec as P
from jax.experimental import pallas as pl
from jax.experimental.pallas import tpu as pltpu

STEPS = 2
current_gain = 0.2
source_gain = 0.5
mixing_side = 0.15
mixing_depth = 0.2
rotation = 0.3
transport = 0.5

LANES = 128
PITCH = 24
LEAD = 8
OCEAN_UNROLL = 4
W, E, N, S = range(4)


def kernel(rows, cols, tiles, mats_count,
           e0, mats, own_h, mask_h, cour_h, stok_h, oc,
           e_out, o_out,
           ebuf, xbuf, low, elow, mbuf, stok, cour, ownv, maskv, obuf,
           sea, o0, o1, ux, uy, drift,
           epack, ehx, ehy, opack, ohx, ohy,
           lsem, esem, ersem, osem, orsem):
    g = lax.axis_index("grp")
    t = lax.axis_index("tile")
    ng = lax.axis_size("grp")
    nt = lax.axis_size("tile")
    bins = tiles * LANES
    points = rows * cols
    has = [g > 0, g < ng - 1, t > 0, t < nt - 1]
    peer = [{"grp": g - 1}, {"grp": g + 1}, {"tile": t - 1}, {"tile": t + 1}]
    back = [E, W, S, N]
    chunks = [(k, min(2, tiles - k)) for k in range(0, tiles, 2)]
    fields = obuf.shape[1]

    def place(m, k):
        full = tiles // 2
        return (m * (full + 1) + k // 2, k % 2) if k < 2 * full else (full, m)

    e4 = ebuf.reshape(tiles, rows + 2, PITCH, LANES)
    o5 = obuf.reshape(2, fields, rows + 2, PITCH, LANES)

    loads = []

    def load(src, dst):
        copy = pltpu.make_async_copy(src, dst, lsem.at[len(loads)])
        copy.start()
        loads.append(copy)
        return copy

    e_load = [load(e0.at[:, :, pl.ds(k * LANES, LANES)], e4.at[k, pl.ds(1, rows), pl.ds(LEAD, cols), :]) for k in range(tiles)]
    small = [load(oc, o5.at[0, :, pl.ds(1, rows), pl.ds(LEAD, cols), :]),
             load(cour_h, cour), load(mask_h, maskv), load(own_h, ownv)]
    m_load = []
    for m in range(mats_count):
        for k in range(0, tiles, 2):
            width = min(2, tiles - k)
            pair, half = place(m, k)
            m_load.append(load(mats.at[m, :, pl.ds(k * LANES, width * LANES)],
                               mbuf.at[pair, :, pl.ds(half * LANES, width * LANES)]))
    stok_load = load(stok_h, stok)

    barrier = pltpu.get_barrier_semaphore()
    for d in range(4):
        @pl.when(has[d])
        def _(d=d):
            pl.semaphore_signal(barrier, inc=1, device_id=peer[d], device_id_type=pl.DeviceIdType.MESH)

    for d in range(4):
        @pl.when(jnp.logical_not(has[d]))
        def _(d=d):
            if d < 2:
                ehx[:, d] = jnp.zeros_like(ehx[:, d])
                ohx[:, d] = jnp.zeros_like(ohx[:, d])
            else:
                ehy[:, d - 2] = jnp.zeros_like(ehy[:, d - 2])
                ohy[:, d - 2] = jnp.zeros_like(ohy[:, d - 2])

    def e_copy(step, d, c):
        k, width = chunks[c]
        span = pl.ds(k, width)
        far = back[d]
        if d < 2:
            src = epack.at[step, d, span]
            dst = ehx.at[step, far, span]
        else:
            src = e4.at[span, 1 if d == N else rows, pl.ds(LEAD, cols), :]
            dst = ehy.at[step, far - 2, span]
        return pltpu.make_async_remote_copy(
            src_ref=src, dst_ref=dst, send_sem=esem.at[step, d, c], recv_sem=ersem.at[step, far, c],
            device_id=peer[d], device_id_type=pl.DeviceIdType.MESH)

    def e_arrival(step, side, c):
        k, width = chunks[c]
        span = pl.ds(k, width)
        dst = ehx.at[step, side, span] if side < 2 else ehy.at[step, side - 2, span]
        return pltpu.make_async_remote_copy(
            src_ref=dst, dst_ref=dst, send_sem=esem.at[step, side, c], recv_sem=ersem.at[step, side, c],
            device_id=peer[side], device_id_type=pl.DeviceIdType.MESH)

    def o_copy(step, d):
        far = back[d]
        if d < 2:
            src = opack.at[step, d]
            dst = ohx.at[step, far]
        else:
            src = o5.at[step, :, 1 if d == N else rows, pl.ds(LEAD, cols), :]
            dst = ohy.at[step, far - 2]
        return pltpu.make_async_remote_copy(
            src_ref=src, dst_ref=dst, send_sem=osem.at[step, d], recv_sem=orsem.at[step, far],
            device_id=peer[d], device_id_type=pl.DeviceIdType.MESH)

    def o_arrival(step, side):
        dst = ohx.at[step, side] if side < 2 else ohy.at[step, side - 2]
        return pltpu.make_async_remote_copy(
            src_ref=dst, dst_ref=dst, send_sem=osem.at[step, side], recv_sem=orsem.at[step, side],
            device_id=peer[side], device_id_type=pl.DeviceIdType.MESH)

    first_col = pl.ds(PITCH + LEAD, rows, stride=PITCH)
    last_col = pl.ds(PITCH + LEAD + cols - 1, rows, stride=PITCH)
    west_col = pl.ds(PITCH + LEAD - 1, rows, stride=PITCH)
    east_col = pl.ds(PITCH + LEAD + cols, rows, stride=PITCH)

    def e_pack(step, c):
        k0, width = chunks[c]
        for k in range(k0, k0 + width):
            epack[step, W, k] = ebuf[k, first_col, :]
            epack[step, E, k] = ebuf[k, last_col, :]

    def o_pack(step):
        for q in range(fields):
            opack[step, W, q] = obuf[step, q, first_col, :]
            opack[step, E, q] = obuf[step, q, last_col, :]

    def send(make):
        for d in range(4):
            @pl.when(has[d])
            def _(d=d):
                make(d).start()

    def wait_recv(make):
        for d in range(4):
            @pl.when(has[d])
            def _(d=d):
                make(d).wait_recv()

    def wait_send(make):
        for d in range(4):
            @pl.when(has[d])
            def _(d=d):
                make(d).wait_send()

    for c, (k0, width) in enumerate(chunks):
        for k in range(k0, k0 + width):
            e_load[k].wait()
        e_pack(0, c)
        if c == 0:
            pl.semaphore_wait(barrier, sum(h.astype(jnp.int32) for h in has))
        send(lambda d: e_copy(0, d, c))
    for copy in small:
        copy.wait()
    o_pack(0)
    send(lambda d: o_copy(0, d))

    mask_all = maskv[...].astype(jnp.float32)
    own_all = ownv[...]
    own0 = jnp.where(own_all == 0, 1.0, 0.0)
    own1 = jnp.where(own_all == 1, 1.0, 0.0)
    for r in range(rows):
        at = pl.ds(r * cols, cols)
        sea[at, :] = jnp.broadcast_to(mask_all[:, r:r + 1], (cols, LANES))
        o0[at, :] = jnp.broadcast_to(own0[:, r:r + 1], (cols, LANES))
        o1[at, :] = jnp.broadcast_to(own1[:, r:r + 1], (cols, LANES))

    def currents(slot):
        for r in range(rows):
            for q, dst in ((0, ux), (1, uy)):
                here = obuf[slot, q, pl.ds((r + 1) * PITCH + LEAD, cols), :]
                dst[r * cols:(r + 1) * cols, :] = current_gain * jnp.broadcast_to(here[:, 0:1], (cols, LANES))

    currents(0)

    def advect(step, k):
        cx = jnp.broadcast_to(cour[0:1, k * LANES:(k + 1) * LANES], (cols, LANES))
        cy = jnp.broadcast_to(cour[1:2, k * LANES:(k + 1) * LANES], (cols, LANES))

        @pl.loop(0, rows // 8)
        def _(block):
            for i in range(8):
                r = block * 8 + i
                base = (r + 1) * PITCH + LEAD
                at = pl.ds(pl.multiple_of(r * cols, cols), cols)
                mid = ebuf[k, pl.ds(base, cols), :]
                west = ebuf[k, pl.ds(base - 1, cols), :]
                east = ebuf[k, pl.ds(base + 1, cols), :]
                north = ebuf[k, pl.ds(base - PITCH, cols), :]
                south = ebuf[k, pl.ds(base + PITCH, cols), :]
                sx = cx + ux[at, :]
                sy = cy + uy[at, :]
                flux = sx * jnp.where(sx > 0.0, mid - west, east - mid)
                flux = flux + sy * jnp.where(sy > 0.0, mid - north, south - mid)
                adv = sea[at, :] * (mid - flux)
                xbuf[k, at, :] = adv
                for m, chosen in ((0, o0), (1, o1)):
                    pair, half = place(m, k)
                    low[pair, at, half * LANES:(half + 1) * LANES] = (adv * chosen[at, :]).astype(jnp.bfloat16)

    lane = lax.broadcasted_iota(jnp.int32, (cols, LANES), 1)

    def ocean(step):
        dst_o = 1 - step

        @pl.loop(0, rows, unroll=OCEAN_UNROLL)
        def _(r):
            base = (r + 1) * PITCH + LEAD
            at = pl.ds(pl.multiple_of(r * cols, cols), cols)
            d0 = drift[at, 0:LANES]
            d1 = drift[at, LANES:2 * LANES]
            sm = sea[at, :]
            mids = [obuf[step, q, pl.ds(base, cols), :] for q in range(fields)]
            for q in range(fields):
                mid = mids[q]
                west = obuf[step, q, pl.ds(base - 1, cols), :]
                east = obuf[step, q, pl.ds(base + 1, cols), :]
                north = obuf[step, q, pl.ds(base - PITCH, cols), :]
                south = obuf[step, q, pl.ds(base + PITCH, cols), :]
                above = jnp.where(lane == LANES - 1, 0.0, pltpu.roll(mid, LANES - 1, 1))
                below = jnp.where(lane == 0, 0.0, pltpu.roll(mid, 1, 1))
                mix = mixing_side * (north + south + west + east - 4.0 * mid) + mixing_depth * (above + below - 2.0 * mid)
                if q == 0:
                    tend = mix + rotation * (mids[1] + d1)
                elif q == 1:
                    tend = mix - rotation * (mids[0] + d0)
                else:
                    tend = mix - transport * (d0 * (0.5 * (east - west)) + d1 * (0.5 * (south - north)))
                new = mid + sm * tend
                if step + 1 < STEPS:
                    obuf[dst_o, q, pl.ds(base, cols), :] = new
                else:
                    o_out[q, r] = new

    for step in range(STEPS):
        for c, (k0, width) in enumerate(chunks):
            wait_recv(lambda d: e_arrival(step, d, c))
            for k in range(k0, k0 + width):
                ebuf[k, west_col, :] = ehx[step, W, k]
                ebuf[k, east_col, :] = ehx[step, E, k]
                ebuf[k, pl.ds(LEAD, cols), :] = ehy[step, 0, k]
                ebuf[k, pl.ds((rows + 1) * PITCH + LEAD, cols), :] = ehy[step, 1, k]
                advect(step, k)
        for c in range(len(chunks)):
            wait_send(lambda d: e_copy(step, d, c))
        for c, (k0, width) in enumerate(chunks):
            if step == 0 and c == 0:
                for copy in m_load:
                    copy.wait()
            src = 0.0
            for pair in range(tiles):
                src = src + lax.dot_general(
                    low[pair], mbuf[pair, k0 * LANES:(k0 + width) * LANES, :], (((1,), (1,)), ((), ())),
                    preferred_element_type=jnp.float32)
            for k in range(k0, k0 + width):
                part = src[:, (k - k0) * LANES:(k - k0 + 1) * LANES]
                new = sea[...] * (xbuf[k] + source_gain * part)
                if step + 1 < STEPS:
                    e4[k, 1:rows + 1, LEAD:LEAD + cols, :] = new.reshape(rows, cols, LANES)
                else:
                    e_out[:, :, k * LANES:(k + 1) * LANES] = new.reshape(rows, cols, LANES)
                elow[:, k * LANES:(k + 1) * LANES] = new.astype(jnp.bfloat16)
            if step + 1 < STEPS:
                e_pack(step + 1, c)
                send(lambda d: e_copy(step + 1, d, c))
        if step == 0:
            stok_load.wait()
        drift[...] = jnp.dot(elow[...], stok[...], preferred_element_type=jnp.float32)
        wait_recv(lambda d: o_arrival(step, d))
        for q in range(fields):
            obuf[step, q, west_col, :] = ohx[step, W, q]
            obuf[step, q, east_col, :] = ohx[step, E, q]
            obuf[step, q, pl.ds(LEAD, cols), :] = ohy[step, 0, q]
            obuf[step, q, pl.ds((rows + 1) * PITCH + LEAD, cols), :] = ohy[step, 1, q]
        if step == 1:
            wait_send(lambda d: o_copy(0, d))
        ocean(step)
        if step + 1 < STEPS:
            currents(1 - step)
            o_pack(step + 1)
            send(lambda d: o_copy(step + 1, d))
    wait_send(lambda d: o_copy(1, d))


def local(spectrum, matrices, ownership, land_mask, courant, stokes_weight, ocean):
    bins, rows, cols = spectrum.shape
    mats = matrices.reshape(matrices.shape[2:])
    count = mats.shape[0]
    tiles = bins // LANES
    points = rows * cols
    fields = ocean.shape[0]
    chunk_count = -(-tiles // 2)
    flat = (rows + 2) * PITCH
    e0 = jnp.transpose(spectrum, (1, 2, 0))
    f32 = jnp.float32
    any_spec = pl.BlockSpec(memory_space=pltpu.HBM)
    e_new, o_new = pl.pallas_call(
        functools.partial(kernel, rows, cols, tiles, count),
        out_shape=(jax.ShapeDtypeStruct((rows, cols, bins), f32), jax.ShapeDtypeStruct(ocean.shape, f32)),
        in_specs=[any_spec] * 7,
        out_specs=(pl.BlockSpec(memory_space=pltpu.VMEM),) * 2,
        scratch_shapes=[
            pltpu.VMEM((tiles, flat, LANES), f32),
            pltpu.VMEM((tiles, points, LANES), f32),
            pltpu.VMEM((tiles, points, 2 * LANES), jnp.bfloat16),
            pltpu.VMEM((points, bins), jnp.bfloat16),
            pltpu.VMEM((tiles, bins, 2 * LANES), jnp.bfloat16),
            pltpu.VMEM((bins, 2 * LANES), jnp.bfloat16),
            pltpu.VMEM((2, bins), f32),
            pltpu.VMEM((cols, rows), jnp.int32),
            pltpu.VMEM((cols, rows), jnp.int32),
            pltpu.VMEM((2, fields, flat, LANES), f32),
        ] + [pltpu.VMEM((points, LANES), f32)] * 5 + [
            pltpu.VMEM((points, 2 * LANES), f32),
            pltpu.VMEM((STEPS, 2, tiles, rows, LANES), f32),
            pltpu.VMEM((STEPS, 2, tiles, rows, LANES), f32),
            pltpu.VMEM((STEPS, 2, tiles, cols, LANES), f32),
            pltpu.VMEM((STEPS, 2, fields, rows, LANES), f32),
            pltpu.VMEM((STEPS, 2, fields, rows, LANES), f32),
            pltpu.VMEM((STEPS, 2, fields, cols, LANES), f32),
            pltpu.SemaphoreType.DMA((tiles + 5 + chunk_count * count,)),
            pltpu.SemaphoreType.DMA((STEPS, 4, chunk_count)),
            pltpu.SemaphoreType.DMA((STEPS, 4, chunk_count)),
            pltpu.SemaphoreType.DMA((STEPS, 4)),
            pltpu.SemaphoreType.DMA((STEPS, 4)),
        ],
        compiler_params=pltpu.CompilerParams(
            collective_id=0, has_side_effects=True, vmem_limit_bytes=34 * 1024 * 1024),
    )(*[pltpu.with_memory_space_constraint(x, pltpu.HBM) for x in (e0, mats, ownership.T, land_mask.T, courant, stokes_weight, ocean)])
    return jnp.transpose(e_new, (2, 0, 1)), o_new


def solution(mesh):
    in_specs = (
        P(None, "tile", "grp"),
        P("tile", "grp", None, None, None),
        P("tile", "grp"),
        P("tile", "grp"),
        P(),
        P(),
        P(None, "tile", "grp", None),
    )
    out_specs = (P(None, "tile", "grp"), P(None, "tile", "grp", None))
    return jax.shard_map(local, mesh=mesh, in_specs=in_specs, out_specs=out_specs, check_vma=False)
```

```python
import functools
import jax
import jax.numpy as jnp
from jax import lax
from jax.sharding import PartitionSpec as P
from jax.experimental import pallas as pl
from jax.experimental.pallas import tpu as pltpu

STEPS = 2
current_gain = 0.2
source_gain = 0.5
mixing_side = 0.15
mixing_depth = 0.2
rotation = 0.3
transport = 0.5

LANES = 128
PITCH = 24
LEAD = 8
OCEAN_UNROLL = 4
W, E, N, S = range(4)


def kernel(rows, cols, tiles, mats_count,
           e0, mats, own_h, mask_h, cour_h, stok_h, oc,
           e_out, o_out,
           ebuf, xbuf, low, elow, mbuf, stok, cour, ownv, maskv, obuf,
           sea, o0, o1, ux, uy, drift,
           epack, ehx, ehy, opack, ohx, ohy,
           lsem, esem, ersem, osem, orsem):
    g = lax.axis_index("grp")
    t = lax.axis_index("tile")
    ng = lax.axis_size("grp")
    nt = lax.axis_size("tile")
    bins = tiles * LANES
    points = rows * cols
    has = [g > 0, g < ng - 1, t > 0, t < nt - 1]
    peer = [{"grp": g - 1}, {"grp": g + 1}, {"tile": t - 1}, {"tile": t + 1}]
    back = [E, W, S, N]
    chunks = [(k, min(2, tiles - k)) for k in range(0, tiles, 2)]
    fields = obuf.shape[1]

    def place(m, k):
        full = tiles // 2
        return (m * (full + 1) + k // 2, k % 2) if k < 2 * full else (full, m)

    e4 = ebuf.reshape(tiles, rows + 2, PITCH, LANES)
    o5 = obuf.reshape(2, fields, rows + 2, PITCH, LANES)

    barrier = pltpu.get_barrier_semaphore()
    for d in range(4):
        @pl.when(has[d])
        def _(d=d):
            pl.semaphore_signal(barrier, inc=1, device_id=peer[d], device_id_type=pl.DeviceIdType.MESH)

    loads = []

    def load(src, dst):
        copy = pltpu.make_async_copy(src, dst, lsem.at[len(loads)])
        copy.start()
        loads.append(copy)
        return copy

    e_load = [load(e0.at[:, :, pl.ds(k * LANES, LANES)], e4.at[k, pl.ds(1, rows), pl.ds(LEAD, cols), :]) for k in range(tiles)]
    small = [load(oc, o5.at[0, :, pl.ds(1, rows), pl.ds(LEAD, cols), :]),
             load(cour_h, cour), load(mask_h, maskv), load(own_h, ownv)]
    for d in range(4):
        @pl.when(jnp.logical_not(has[d]))
        def _(d=d):
            if d < 2:
                ehx[:, d] = jnp.zeros_like(ehx[:, d])
                ohx[:, d] = jnp.zeros_like(ohx[:, d])
            else:
                ehy[:, d - 2] = jnp.zeros_like(ehy[:, d - 2])
                ohy[:, d - 2] = jnp.zeros_like(ohy[:, d - 2])

    def e_copy(step, d, c):
        k, width = chunks[c]
        span = pl.ds(k, width)
        far = back[d]
        if d < 2:
            src = epack.at[step, d, span]
            dst = ehx.at[step, far, span]
        else:
            src = e4.at[span, 1 if d == N else rows, pl.ds(LEAD, cols), :]
            dst = ehy.at[step, far - 2, span]
        return pltpu.make_async_remote_copy(
            src_ref=src, dst_ref=dst, send_sem=esem.at[step, d, c], recv_sem=ersem.at[step, far, c],
            device_id=peer[d], device_id_type=pl.DeviceIdType.MESH)

    def e_arrival(step, side, c):
        k, width = chunks[c]
        span = pl.ds(k, width)
        dst = ehx.at[step, side, span] if side < 2 else ehy.at[step, side - 2, span]
        return pltpu.make_async_remote_copy(
            src_ref=dst, dst_ref=dst, send_sem=esem.at[step, side, c], recv_sem=ersem.at[step, side, c],
            device_id=peer[side], device_id_type=pl.DeviceIdType.MESH)

    def o_copy(step, d):
        far = back[d]
        if d < 2:
            src = opack.at[step, d]
            dst = ohx.at[step, far]
        else:
            src = o5.at[step, :, 1 if d == N else rows, pl.ds(LEAD, cols), :]
            dst = ohy.at[step, far - 2]
        return pltpu.make_async_remote_copy(
            src_ref=src, dst_ref=dst, send_sem=osem.at[step, d], recv_sem=orsem.at[step, far],
            device_id=peer[d], device_id_type=pl.DeviceIdType.MESH)

    def o_arrival(step, side):
        dst = ohx.at[step, side] if side < 2 else ohy.at[step, side - 2]
        return pltpu.make_async_remote_copy(
            src_ref=dst, dst_ref=dst, send_sem=osem.at[step, side], recv_sem=orsem.at[step, side],
            device_id=peer[side], device_id_type=pl.DeviceIdType.MESH)

    first_col = pl.ds(PITCH + LEAD, rows, stride=PITCH)
    last_col = pl.ds(PITCH + LEAD + cols - 1, rows, stride=PITCH)
    west_col = pl.ds(PITCH + LEAD - 1, rows, stride=PITCH)
    east_col = pl.ds(PITCH + LEAD + cols, rows, stride=PITCH)

    def e_pack(step, c):
        k0, width = chunks[c]
        for k in range(k0, k0 + width):
            epack[step, W, k] = ebuf[k, first_col, :]
            epack[step, E, k] = ebuf[k, last_col, :]

    def o_pack(step):
        for q in range(fields):
            opack[step, W, q] = obuf[step, q, first_col, :]
            opack[step, E, q] = obuf[step, q, last_col, :]

    def send(make):
        for d in (N, S, W, E):
            @pl.when(has[d])
            def _(d=d):
                make(d).start()

    def wait_recv(make):
        for d in range(4):
            @pl.when(has[d])
            def _(d=d):
                make(d).wait_recv()

    def wait_send(make):
        for d in range(4):
            @pl.when(has[d])
            def _(d=d):
                make(d).wait_send()

    for c, (k0, width) in enumerate(chunks):
        for k in range(k0, k0 + width):
            e_load[k].wait()
        e_pack(0, c)
    m_load = []
    for m in range(mats_count):
        for k in range(0, tiles, 2):
            width = min(2, tiles - k)
            pair, half = place(m, k)
            m_load.append(load(mats.at[m, :, pl.ds(k * LANES, width * LANES)],
                               mbuf.at[pair, :, pl.ds(half * LANES, width * LANES)]))
    stok_load = load(stok_h, stok)
    pl.semaphore_wait(barrier, sum(h.astype(jnp.int32) for h in has))
    for c in range(len(chunks)):
        send(lambda d: e_copy(0, d, c))
    for copy in small:
        copy.wait()
    o_pack(0)
    send(lambda d: o_copy(0, d))

    mask_all = maskv[...].astype(jnp.float32)
    own_all = ownv[...]
    own0 = jnp.where(own_all == 0, 1.0, 0.0)
    own1 = jnp.where(own_all == 1, 1.0, 0.0)
    for r in range(rows):
        at = pl.ds(r * cols, cols)
        sea[at, :] = jnp.broadcast_to(mask_all[:, r:r + 1], (cols, LANES))
        o0[at, :] = jnp.broadcast_to(own0[:, r:r + 1], (cols, LANES))
        o1[at, :] = jnp.broadcast_to(own1[:, r:r + 1], (cols, LANES))

    def currents(slot):
        for r in range(rows):
            for q, dst in ((0, ux), (1, uy)):
                here = obuf[slot, q, pl.ds((r + 1) * PITCH + LEAD, cols), :]
                dst[r * cols:(r + 1) * cols, :] = current_gain * jnp.broadcast_to(here[:, 0:1], (cols, LANES))

    currents(0)

    def advect(k, base, at, stride=None):
        count = cols if stride is None else rows

        def near(shift):
            return ebuf[k, pl.ds(base + shift, count, stride=None if stride is None else PITCH), :]

        cx = jnp.broadcast_to(cour[0:1, k * LANES:(k + 1) * LANES], (count, LANES))
        cy = jnp.broadcast_to(cour[1:2, k * LANES:(k + 1) * LANES], (count, LANES))
        mid = near(0)
        sx = cx + ux[at, :]
        sy = cy + uy[at, :]
        flux = sx * jnp.where(sx > 0.0, mid - near(-1), near(1) - mid)
        flux = flux + sy * jnp.where(sy > 0.0, mid - near(-PITCH), near(PITCH) - mid)
        xbuf[k, at, :] = sea[at, :] * (mid - flux)

    def advect_all(k):
        @pl.loop(0, rows // 8)
        def _(block):
            for i in range(8):
                r = block * 8 + i
                advect(k, (r + 1) * PITCH + LEAD, pl.ds(pl.multiple_of(r * cols, cols), cols))

    def advect_border(k):
        for r in (0, rows - 1):
            advect(k, (r + 1) * PITCH + LEAD, pl.ds(r * cols, cols))
        for c in (0, cols - 1):
            advect(k, PITCH + LEAD + c, pl.ds(c, rows, stride=cols), cols)

    def lower(k):
        @pl.loop(0, rows // 8)
        def _(block):
            for i in range(8):
                at = pl.ds(pl.multiple_of((block * 8 + i) * cols, cols), cols)
                adv = xbuf[k, at, :]
                for m, chosen in ((0, o0), (1, o1)):
                    pair, half = place(m, k)
                    low[pair, at, half * LANES:(half + 1) * LANES] = (adv * chosen[at, :]).astype(jnp.bfloat16)

    lane = lax.broadcasted_iota(jnp.int32, (cols, LANES), 1)

    def ocean(step):
        dst_o = 1 - step

        @pl.loop(0, rows, unroll=OCEAN_UNROLL)
        def _(r):
            base = (r + 1) * PITCH + LEAD
            at = pl.ds(pl.multiple_of(r * cols, cols), cols)
            d0 = drift[at, 0:LANES]
            d1 = drift[at, LANES:2 * LANES]
            sm = sea[at, :]
            mids = [obuf[step, q, pl.ds(base, cols), :] for q in range(fields)]
            for q in range(fields):
                mid = mids[q]
                west = obuf[step, q, pl.ds(base - 1, cols), :]
                east = obuf[step, q, pl.ds(base + 1, cols), :]
                north = obuf[step, q, pl.ds(base - PITCH, cols), :]
                south = obuf[step, q, pl.ds(base + PITCH, cols), :]
                above = jnp.where(lane == LANES - 1, 0.0, pltpu.roll(mid, LANES - 1, 1))
                below = jnp.where(lane == 0, 0.0, pltpu.roll(mid, 1, 1))
                mix = mixing_side * (north + south + west + east - 4.0 * mid) + mixing_depth * (above + below - 2.0 * mid)
                if q == 0:
                    tend = mix + rotation * (mids[1] + d1)
                elif q == 1:
                    tend = mix - rotation * (mids[0] + d0)
                else:
                    tend = mix - transport * (d0 * (0.5 * (east - west)) + d1 * (0.5 * (south - north)))
                new = mid + sm * tend
                if step + 1 < STEPS:
                    obuf[dst_o, q, pl.ds(base, cols), :] = new
                else:
                    o_out[q, r] = new

    for step in range(STEPS):
        for k in range(tiles):
            advect_all(k)
        for c, (k0, width) in enumerate(chunks):
            wait_recv(lambda d: e_arrival(step, d, c))
            for k in range(k0, k0 + width):
                ebuf[k, west_col, :] = ehx[step, W, k]
                ebuf[k, east_col, :] = ehx[step, E, k]
                ebuf[k, pl.ds(LEAD, cols), :] = ehy[step, 0, k]
                ebuf[k, pl.ds((rows + 1) * PITCH + LEAD, cols), :] = ehy[step, 1, k]
                advect_border(k)
                lower(k)
        for c in range(len(chunks)):
            wait_send(lambda d: e_copy(step, d, c))
        for c, (k0, width) in enumerate(chunks):
            if step == 0 and c == 0:
                for copy in m_load:
                    copy.wait()
            src = 0.0
            for pair in range(tiles):
                src = src + lax.dot_general(
                    low[pair], mbuf[pair, k0 * LANES:(k0 + width) * LANES, :], (((1,), (1,)), ((), ())),
                    preferred_element_type=jnp.float32)
            for k in range(k0, k0 + width):
                part = src[:, (k - k0) * LANES:(k - k0 + 1) * LANES]
                new = sea[...] * (xbuf[k] + source_gain * part)
                if step + 1 < STEPS:
                    e4[k, 1:rows + 1, LEAD:LEAD + cols, :] = new.reshape(rows, cols, LANES)
                else:
                    e_out[:, :, k * LANES:(k + 1) * LANES] = new.reshape(rows, cols, LANES)
                elow[:, k * LANES:(k + 1) * LANES] = new.astype(jnp.bfloat16)
            if step + 1 < STEPS:
                e_pack(step + 1, c)
                send(lambda d: e_copy(step + 1, d, c))
        if step == 0:
            stok_load.wait()
        drift[...] = jnp.dot(elow[...], stok[...], preferred_element_type=jnp.float32)
        wait_recv(lambda d: o_arrival(step, d))
        for q in range(fields):
            obuf[step, q, west_col, :] = ohx[step, W, q]
            obuf[step, q, east_col, :] = ohx[step, E, q]
            obuf[step, q, pl.ds(LEAD, cols), :] = ohy[step, 0, q]
            obuf[step, q, pl.ds((rows + 1) * PITCH + LEAD, cols), :] = ohy[step, 1, q]
        if step == 1:
            wait_send(lambda d: o_copy(0, d))
        ocean(step)
        if step + 1 < STEPS:
            currents(1 - step)
            o_pack(step + 1)
            send(lambda d: o_copy(step + 1, d))
    wait_send(lambda d: o_copy(1, d))


def local(spectrum, matrices, ownership, land_mask, courant, stokes_weight, ocean):
    bins, rows, cols = spectrum.shape
    mats = matrices.reshape(matrices.shape[2:])
    count = mats.shape[0]
    tiles = bins // LANES
    points = rows * cols
    fields = ocean.shape[0]
    chunk_count = -(-tiles // 2)
    flat = (rows + 2) * PITCH
    e0 = jnp.transpose(spectrum, (1, 2, 0))
    f32 = jnp.float32
    any_spec = pl.BlockSpec(memory_space=pltpu.HBM)
    e_new, o_new = pl.pallas_call(
        functools.partial(kernel, rows, cols, tiles, count),
        out_shape=(jax.ShapeDtypeStruct((rows, cols, bins), f32), jax.ShapeDtypeStruct(ocean.shape, f32)),
        in_specs=[any_spec] * 7,
        out_specs=(pl.BlockSpec(memory_space=pltpu.VMEM),) * 2,
        scratch_shapes=[
            pltpu.VMEM((tiles, flat, LANES), f32),
            pltpu.VMEM((tiles, points, LANES), f32),
            pltpu.VMEM((tiles, points, 2 * LANES), jnp.bfloat16),
            pltpu.VMEM((points, bins), jnp.bfloat16),
            pltpu.VMEM((tiles, bins, 2 * LANES), jnp.bfloat16),
            pltpu.VMEM((bins, 2 * LANES), jnp.bfloat16),
            pltpu.VMEM((2, bins), f32),
            pltpu.VMEM((cols, rows), jnp.int32),
            pltpu.VMEM((cols, rows), jnp.int32),
            pltpu.VMEM((2, fields, flat, LANES), f32),
        ] + [pltpu.VMEM((points, LANES), f32)] * 5 + [
            pltpu.VMEM((points, 2 * LANES), f32),
            pltpu.VMEM((STEPS, 2, tiles, rows, LANES), f32),
            pltpu.VMEM((STEPS, 2, tiles, rows, LANES), f32),
            pltpu.VMEM((STEPS, 2, tiles, cols, LANES), f32),
            pltpu.VMEM((STEPS, 2, fields, rows, LANES), f32),
            pltpu.VMEM((STEPS, 2, fields, rows, LANES), f32),
            pltpu.VMEM((STEPS, 2, fields, cols, LANES), f32),
            pltpu.SemaphoreType.DMA((tiles + 5 + chunk_count * count,)),
            pltpu.SemaphoreType.DMA((STEPS, 4, chunk_count)),
            pltpu.SemaphoreType.DMA((STEPS, 4, chunk_count)),
            pltpu.SemaphoreType.DMA((STEPS, 4)),
            pltpu.SemaphoreType.DMA((STEPS, 4)),
        ],
        compiler_params=pltpu.CompilerParams(
            collective_id=0, has_side_effects=True, vmem_limit_bytes=34 * 1024 * 1024),
    )(*[pltpu.with_memory_space_constraint(x, pltpu.HBM) for x in (e0, mats, ownership.T, land_mask.T, courant, stokes_weight, ocean)])
    return jnp.transpose(e_new, (2, 0, 1)), o_new


def solution(mesh):
    in_specs = (
        P(None, "tile", "grp"),
        P("tile", "grp", None, None, None),
        P("tile", "grp"),
        P("tile", "grp"),
        P(),
        P(),
        P(None, "tile", "grp", None),
    )
    out_specs = (P(None, "tile", "grp"), P(None, "tile", "grp", None))
    return jax.shard_map(local, mesh=mesh, in_specs=in_specs, out_specs=out_specs, check_vma=False)
```

```python
import functools
import jax
import jax.numpy as jnp
from jax import lax
from jax.sharding import PartitionSpec as P
from jax.experimental import pallas as pl
from jax.experimental.pallas import tpu as pltpu

STEPS = 2
current_gain = 0.2
source_gain = 0.5
mixing_side = 0.15
mixing_depth = 0.2
rotation = 0.3
transport = 0.5

LANES = 128
PITCH = 24
LEAD = 8
OCEAN_UNROLL = 4
W, E, N, S = range(4)


def ocean_rows(obuf, drift, sea, first, last, cols, put):
    fields = obuf.shape[0]
    lane = lax.broadcasted_iota(jnp.int32, (cols, LANES), 1)

    @pl.loop(first, last, unroll=OCEAN_UNROLL)
    def _(r):
        base = (r + 1) * PITCH + LEAD
        at = pl.ds(pl.multiple_of(r * cols, cols), cols)
        d0 = drift[at, 0:LANES]
        d1 = drift[at, LANES:2 * LANES]
        sm = sea[at, :]
        mids = [obuf[q, pl.ds(base, cols), :] for q in range(fields)]
        for q in range(fields):
            mid = mids[q]
            west = obuf[q, pl.ds(base - 1, cols), :]
            east = obuf[q, pl.ds(base + 1, cols), :]
            north = obuf[q, pl.ds(base - PITCH, cols), :]
            south = obuf[q, pl.ds(base + PITCH, cols), :]
            above = jnp.where(lane == LANES - 1, 0.0, pltpu.roll(mid, LANES - 1, 1))
            below = jnp.where(lane == 0, 0.0, pltpu.roll(mid, 1, 1))
            mix = mixing_side * (north + south + west + east - 4.0 * mid) + mixing_depth * (above + below - 2.0 * mid)
            if q == 0:
                tend = mix + rotation * (mids[1] + d1)
            elif q == 1:
                tend = mix - rotation * (mids[0] + d0)
            else:
                tend = mix - transport * (d0 * (0.5 * (east - west)) + d1 * (0.5 * (south - north)))
            put(q, r, at, base, mid + sm * tend)


def last_kernel(rows, cols, e_new, obuf, drift, sea, e_out, o_out, stage, sem):
    copies = []
    blocks = 4
    size = rows // blocks

    def out(src, dst):
        copy = pltpu.make_async_copy(src, dst, sem.at[len(copies)])
        copy.start()
        copies.append(copy)

    def put(q, r, at, base, new):
        stage[q, r] = new

    for i in range(blocks):
        span = pl.ds(i * size, size)
        out(e_new.at[span], e_out.at[span])
    for i in range(blocks):
        span = pl.ds(i * size, size)
        ocean_rows(obuf, drift, sea, i * size, (i + 1) * size, cols, put)
        out(stage.at[:, span], o_out.at[:, span])
    for copy in copies:
        copy.wait()


def kernel(rows, cols, tiles, mats_count,
           e0, mats, own_h, mask_h, cour_h, stok_h, oc,
           e_out, obuf1, drift, sea,
           ebuf, xbuf, low, elow, mbuf, stok, cour, ownv, maskv, obuf0,
           o0, o1, ux, uy,
           epack, ehx, ehy, opack, ohx, ohy,
           lsem, esem, ersem, osem, orsem):
    g = lax.axis_index("grp")
    t = lax.axis_index("tile")
    ng = lax.axis_size("grp")
    nt = lax.axis_size("tile")
    bins = tiles * LANES
    points = rows * cols
    has = [g > 0, g < ng - 1, t > 0, t < nt - 1]
    peer = [{"grp": g - 1}, {"grp": g + 1}, {"tile": t - 1}, {"tile": t + 1}]
    back = [E, W, S, N]
    chunks = [(k, min(2, tiles - k)) for k in range(0, tiles, 2)]
    obuf = (obuf0, obuf1)
    fields = obuf0.shape[0]

    def place(m, k):
        full = tiles // 2
        return (m * (full + 1) + k // 2, k % 2) if k < 2 * full else (full, m)

    e4 = ebuf.reshape(tiles, rows + 2, PITCH, LANES)
    o4 = [o.reshape(fields, rows + 2, PITCH, LANES) for o in obuf]

    barrier = pltpu.get_barrier_semaphore()
    for d in range(4):
        @pl.when(has[d])
        def _(d=d):
            pl.semaphore_signal(barrier, inc=1, device_id=peer[d], device_id_type=pl.DeviceIdType.MESH)

    loads = []

    def load(src, dst):
        copy = pltpu.make_async_copy(src, dst, lsem.at[len(loads)])
        copy.start()
        loads.append(copy)
        return copy

    e_load = [load(e0.at[:, :, pl.ds(k * LANES, LANES)], e4.at[k, pl.ds(1, rows), pl.ds(LEAD, cols), :]) for k in range(tiles)]
    small = [load(oc, o4[0].at[:, pl.ds(1, rows), pl.ds(LEAD, cols), :]),
             load(cour_h, cour), load(mask_h, maskv), load(own_h, ownv)]
    for d in range(4):
        @pl.when(jnp.logical_not(has[d]))
        def _(d=d):
            if d < 2:
                ehx[:, d] = jnp.zeros_like(ehx[:, d])
                ohx[:, d] = jnp.zeros_like(ohx[:, d])
            else:
                ehy[:, d - 2] = jnp.zeros_like(ehy[:, d - 2])
                ohy[:, d - 2] = jnp.zeros_like(ohy[:, d - 2])

    def e_copy(step, d, c):
        k, width = chunks[c]
        span = pl.ds(k, width)
        far = back[d]
        if d < 2:
            src = epack.at[step, d, span]
            dst = ehx.at[step, far, span]
        else:
            src = e4.at[span, 1 if d == N else rows, pl.ds(LEAD, cols), :]
            dst = ehy.at[step, far - 2, span]
        return pltpu.make_async_remote_copy(
            src_ref=src, dst_ref=dst, send_sem=esem.at[step, d, c], recv_sem=ersem.at[step, far, c],
            device_id=peer[d], device_id_type=pl.DeviceIdType.MESH)

    def e_arrival(step, side, c):
        k, width = chunks[c]
        span = pl.ds(k, width)
        dst = ehx.at[step, side, span] if side < 2 else ehy.at[step, side - 2, span]
        return pltpu.make_async_remote_copy(
            src_ref=dst, dst_ref=dst, send_sem=esem.at[step, side, c], recv_sem=ersem.at[step, side, c],
            device_id=peer[side], device_id_type=pl.DeviceIdType.MESH)

    def o_copy(step, d):
        far = back[d]
        if d < 2:
            src = opack.at[step, d]
            dst = ohx.at[step, far]
        else:
            src = o4[step].at[:, 1 if d == N else rows, pl.ds(LEAD, cols), :]
            dst = ohy.at[step, far - 2]
        return pltpu.make_async_remote_copy(
            src_ref=src, dst_ref=dst, send_sem=osem.at[step, d], recv_sem=orsem.at[step, far],
            device_id=peer[d], device_id_type=pl.DeviceIdType.MESH)

    def o_arrival(step, side):
        dst = ohx.at[step, side] if side < 2 else ohy.at[step, side - 2]
        return pltpu.make_async_remote_copy(
            src_ref=dst, dst_ref=dst, send_sem=osem.at[step, side], recv_sem=orsem.at[step, side],
            device_id=peer[side], device_id_type=pl.DeviceIdType.MESH)

    first_col = pl.ds(PITCH + LEAD, rows, stride=PITCH)
    last_col = pl.ds(PITCH + LEAD + cols - 1, rows, stride=PITCH)
    west_col = pl.ds(PITCH + LEAD - 1, rows, stride=PITCH)
    east_col = pl.ds(PITCH + LEAD + cols, rows, stride=PITCH)

    def e_pack(step, c):
        k0, width = chunks[c]
        for k in range(k0, k0 + width):
            epack[step, W, k] = ebuf[k, first_col, :]
            epack[step, E, k] = ebuf[k, last_col, :]

    def o_pack(step):
        for q in range(fields):
            opack[step, W, q] = obuf[step][q, first_col, :]
            opack[step, E, q] = obuf[step][q, last_col, :]

    def send(make):
        for d in (N, S, W, E):
            @pl.when(has[d])
            def _(d=d):
                make(d).start()

    def wait_recv(make):
        for d in range(4):
            @pl.when(has[d])
            def _(d=d):
                make(d).wait_recv()

    def wait_send(make):
        for d in range(4):
            @pl.when(has[d])
            def _(d=d):
                make(d).wait_send()

    for c, (k0, width) in enumerate(chunks):
        for k in range(k0, k0 + width):
            e_load[k].wait()
        e_pack(0, c)
    m_load = []
    for m in range(mats_count):
        for k in range(0, tiles, 2):
            width = min(2, tiles - k)
            pair, half = place(m, k)
            m_load.append(load(mats.at[m, :, pl.ds(k * LANES, width * LANES)],
                               mbuf.at[pair, :, pl.ds(half * LANES, width * LANES)]))
    stok_load = load(stok_h, stok)
    pl.semaphore_wait(barrier, sum(h.astype(jnp.int32) for h in has))
    for c in range(len(chunks)):
        send(lambda d: e_copy(0, d, c))
    for copy in small:
        copy.wait()
    o_pack(0)
    send(lambda d: o_copy(0, d))

    mask_all = maskv[...].astype(jnp.float32)
    own_all = ownv[...]
    own0 = jnp.where(own_all == 0, 1.0, 0.0)
    own1 = jnp.where(own_all == 1, 1.0, 0.0)
    for r in range(rows):
        at = pl.ds(r * cols, cols)
        sea[at, :] = jnp.broadcast_to(mask_all[:, r:r + 1], (cols, LANES))
        o0[at, :] = jnp.broadcast_to(own0[:, r:r + 1], (cols, LANES))
        o1[at, :] = jnp.broadcast_to(own1[:, r:r + 1], (cols, LANES))

    def currents(slot):
        for r in range(rows):
            for q, dst in ((0, ux), (1, uy)):
                here = obuf[slot][q, pl.ds((r + 1) * PITCH + LEAD, cols), :]
                dst[r * cols:(r + 1) * cols, :] = current_gain * jnp.broadcast_to(here[:, 0:1], (cols, LANES))

    currents(0)

    def advect(k, base, at, stride=None):
        count = cols if stride is None else rows

        def near(shift):
            return ebuf[k, pl.ds(base + shift, count, stride=None if stride is None else PITCH), :]

        cx = jnp.broadcast_to(cour[0:1, k * LANES:(k + 1) * LANES], (count, LANES))
        cy = jnp.broadcast_to(cour[1:2, k * LANES:(k + 1) * LANES], (count, LANES))
        mid = near(0)
        sx = cx + ux[at, :]
        sy = cy + uy[at, :]
        flux = sx * jnp.where(sx > 0.0, mid - near(-1), near(1) - mid)
        flux = flux + sy * jnp.where(sy > 0.0, mid - near(-PITCH), near(PITCH) - mid)
        xbuf[k, at, :] = sea[at, :] * (mid - flux)

    def advect_all(k):
        @pl.loop(0, rows // 8)
        def _(block):
            for i in range(8):
                r = block * 8 + i
                advect(k, (r + 1) * PITCH + LEAD, pl.ds(pl.multiple_of(r * cols, cols), cols))

    def advect_border(k):
        for r in (0, rows - 1):
            advect(k, (r + 1) * PITCH + LEAD, pl.ds(r * cols, cols))
        for c in (0, cols - 1):
            advect(k, PITCH + LEAD + c, pl.ds(c, rows, stride=cols), cols)

    def lower(k):
        @pl.loop(0, rows // 8)
        def _(block):
            for i in range(8):
                at = pl.ds(pl.multiple_of((block * 8 + i) * cols, cols), cols)
                adv = xbuf[k, at, :]
                for m, chosen in ((0, o0), (1, o1)):
                    pair, half = place(m, k)
                    low[pair, at, half * LANES:(half + 1) * LANES] = (adv * chosen[at, :]).astype(jnp.bfloat16)

    def put(q, base, new):
        obuf[1][q, pl.ds(base, cols), :] = new

    for step in range(STEPS):
        for k in range(tiles):
            advect_all(k)
        for c, (k0, width) in enumerate(chunks):
            wait_recv(lambda d: e_arrival(step, d, c))
            for k in range(k0, k0 + width):
                ebuf[k, west_col, :] = ehx[step, W, k]
                ebuf[k, east_col, :] = ehx[step, E, k]
                ebuf[k, pl.ds(LEAD, cols), :] = ehy[step, 0, k]
                ebuf[k, pl.ds((rows + 1) * PITCH + LEAD, cols), :] = ehy[step, 1, k]
                advect_border(k)
                lower(k)
        for c in range(len(chunks)):
            wait_send(lambda d: e_copy(step, d, c))
        for c, (k0, width) in enumerate(chunks):
            if step == 0 and c == 0:
                for copy in m_load:
                    copy.wait()
            src = 0.0
            for pair in range(tiles):
                src = src + lax.dot_general(
                    low[pair], mbuf[pair, k0 * LANES:(k0 + width) * LANES, :], (((1,), (1,)), ((), ())),
                    preferred_element_type=jnp.float32)
            for k in range(k0, k0 + width):
                part = src[:, (k - k0) * LANES:(k - k0 + 1) * LANES]
                new = sea[...] * (xbuf[k] + source_gain * part)
                if step + 1 < STEPS:
                    e4[k, 1:rows + 1, LEAD:LEAD + cols, :] = new.reshape(rows, cols, LANES)
                else:
                    e_out[:, :, k * LANES:(k + 1) * LANES] = new.reshape(rows, cols, LANES)
                elow[:, k * LANES:(k + 1) * LANES] = new.astype(jnp.bfloat16)
            if step + 1 < STEPS:
                e_pack(step + 1, c)
                send(lambda d: e_copy(step + 1, d, c))
        if step == 0:
            stok_load.wait()
        drift[...] = jnp.dot(elow[...], stok[...], preferred_element_type=jnp.float32)
        wait_recv(lambda d: o_arrival(step, d))
        for q in range(fields):
            obuf[step][q, west_col, :] = ohx[step, W, q]
            obuf[step][q, east_col, :] = ohx[step, E, q]
            obuf[step][q, pl.ds(LEAD, cols), :] = ohy[step, 0, q]
            obuf[step][q, pl.ds((rows + 1) * PITCH + LEAD, cols), :] = ohy[step, 1, q]
        if step == 1:
            wait_send(lambda d: o_copy(0, d))
        if step + 1 < STEPS:
            ocean_rows(obuf[0], drift, sea, 0, rows, cols, lambda q, r, at, base, new: put(q, base, new))
            currents(1 - step)
            o_pack(step + 1)
            send(lambda d: o_copy(step + 1, d))
    wait_send(lambda d: o_copy(1, d))


def local(spectrum, matrices, ownership, land_mask, courant, stokes_weight, ocean):
    bins, rows, cols = spectrum.shape
    mats = matrices.reshape(matrices.shape[2:])
    count = mats.shape[0]
    tiles = bins // LANES
    points = rows * cols
    fields = ocean.shape[0]
    chunk_count = -(-tiles // 2)
    flat = (rows + 2) * PITCH
    e0 = jnp.transpose(spectrum, (1, 2, 0))
    f32 = jnp.float32
    any_spec = pl.BlockSpec(memory_space=pltpu.HBM)
    e_new, o_mid, drift, sea = pl.pallas_call(
        functools.partial(kernel, rows, cols, tiles, count),
        out_shape=(jax.ShapeDtypeStruct((rows, cols, bins), f32), jax.ShapeDtypeStruct((fields, flat, LANES), f32),
                   jax.ShapeDtypeStruct((points, 2 * LANES), f32), jax.ShapeDtypeStruct((points, LANES), f32)),
        in_specs=[any_spec] * 7,
        out_specs=(pl.BlockSpec(memory_space=pltpu.VMEM),) * 4,
        scratch_shapes=[
            pltpu.VMEM((tiles, flat, LANES), f32),
            pltpu.VMEM((tiles, points, LANES), f32),
            pltpu.VMEM((tiles, points, 2 * LANES), jnp.bfloat16),
            pltpu.VMEM((points, bins), jnp.bfloat16),
            pltpu.VMEM((tiles, bins, 2 * LANES), jnp.bfloat16),
            pltpu.VMEM((bins, 2 * LANES), jnp.bfloat16),
            pltpu.VMEM((2, bins), f32),
            pltpu.VMEM((cols, rows), jnp.int32),
            pltpu.VMEM((cols, rows), jnp.int32),
            pltpu.VMEM((fields, flat, LANES), f32),
        ] + [pltpu.VMEM((points, LANES), f32)] * 4 + [
            pltpu.VMEM((STEPS, 2, tiles, rows, LANES), f32),
            pltpu.VMEM((STEPS, 2, tiles, rows, LANES), f32),
            pltpu.VMEM((STEPS, 2, tiles, cols, LANES), f32),
            pltpu.VMEM((STEPS, 2, fields, rows, LANES), f32),
            pltpu.VMEM((STEPS, 2, fields, rows, LANES), f32),
            pltpu.VMEM((STEPS, 2, fields, cols, LANES), f32),
            pltpu.SemaphoreType.DMA((tiles + 5 + chunk_count * count,)),
            pltpu.SemaphoreType.DMA((STEPS, 4, chunk_count)),
            pltpu.SemaphoreType.DMA((STEPS, 4, chunk_count)),
            pltpu.SemaphoreType.DMA((STEPS, 4)),
            pltpu.SemaphoreType.DMA((STEPS, 4)),
        ],
        compiler_params=pltpu.CompilerParams(
            collective_id=0, has_side_effects=True, vmem_limit_bytes=34 * 1024 * 1024),
    )(*[pltpu.with_memory_space_constraint(x, pltpu.HBM) for x in (e0, mats, ownership.T, land_mask.T, courant, stokes_weight, ocean)])
    e_out, o_new = pl.pallas_call(
        functools.partial(last_kernel, rows, cols),
        out_shape=(jax.ShapeDtypeStruct((rows, cols, bins), f32), jax.ShapeDtypeStruct(ocean.shape, f32)),
        in_specs=[pl.BlockSpec(memory_space=pltpu.VMEM)] * 4,
        out_specs=(any_spec, any_spec),
        scratch_shapes=[pltpu.VMEM(ocean.shape, f32), pltpu.SemaphoreType.DMA((8,))],
        compiler_params=pltpu.CompilerParams(vmem_limit_bytes=16 * 1024 * 1024),
    )(e_new, o_mid, drift, sea)
    return jnp.transpose(e_out, (2, 0, 1)), o_new


def solution(mesh):
    in_specs = (
        P(None, "tile", "grp"),
        P("tile", "grp", None, None, None),
        P("tile", "grp"),
        P("tile", "grp"),
        P(),
        P(),
        P(None, "tile", "grp", None),
    )
    out_specs = (P(None, "tile", "grp"), P(None, "tile", "grp", None))
    return jax.shard_map(local, mesh=mesh, in_specs=in_specs, out_specs=out_specs, check_vma=False)
```

```python
import functools
import jax
import jax.numpy as jnp
from jax import lax
from jax.sharding import PartitionSpec as P
from jax.experimental import pallas as pl
from jax.experimental.pallas import tpu as pltpu

STEPS = 2
current_gain = 0.2
source_gain = 0.5
mixing_side = 0.15
mixing_depth = 0.2
rotation = 0.3
transport = 0.5

LANES = 128
PITCH = 24
LEAD = 8
OCEAN_UNROLL = 4
W, E, N, S = range(4)


def ocean_rows(obuf, drift, sea, first, last, cols, put):
    fields = obuf.shape[0]
    lane = lax.broadcasted_iota(jnp.int32, (cols, LANES), 1)

    @pl.loop(first, last, unroll=OCEAN_UNROLL)
    def _(r):
        base = (r + 1) * PITCH + LEAD
        at = pl.ds(pl.multiple_of(r * cols, cols), cols)
        d0 = drift[at, 0:LANES]
        d1 = drift[at, LANES:2 * LANES]
        sm = sea[at, :]
        mids = [obuf[q, pl.ds(base, cols), :] for q in range(fields)]
        for q in range(fields):
            mid = mids[q]
            west = obuf[q, pl.ds(base - 1, cols), :]
            east = obuf[q, pl.ds(base + 1, cols), :]
            north = obuf[q, pl.ds(base - PITCH, cols), :]
            south = obuf[q, pl.ds(base + PITCH, cols), :]
            above = jnp.where(lane == LANES - 1, 0.0, pltpu.roll(mid, LANES - 1, 1))
            below = jnp.where(lane == 0, 0.0, pltpu.roll(mid, 1, 1))
            mix = mixing_side * (north + south + west + east - 4.0 * mid) + mixing_depth * (above + below - 2.0 * mid)
            if q == 0:
                tend = mix + rotation * (mids[1] + d1)
            elif q == 1:
                tend = mix - rotation * (mids[0] + d0)
            else:
                tend = mix - transport * (d0 * (0.5 * (east - west)) + d1 * (0.5 * (south - north)))
            put(q, r, at, base, mid + sm * tend)


def last_kernel(rows, cols, e_new, obuf, drift, sea, e_out, o_out, stage, sem):
    copies = []
    blocks = 4
    size = rows // blocks

    def out(src, dst):
        copy = pltpu.make_async_copy(src, dst, sem.at[len(copies)])
        copy.start()
        copies.append(copy)

    def put(q, r, at, base, new):
        stage[q, r] = new

    for i in range(blocks):
        span = pl.ds(i * size, size)
        out(e_new.at[span], e_out.at[span])
    for i in range(blocks):
        span = pl.ds(i * size, size)
        ocean_rows(obuf, drift, sea, i * size, (i + 1) * size, cols, put)
        out(stage.at[:, span], o_out.at[:, span])
    for copy in copies:
        copy.wait()


def kernel(rows, cols, tiles, mats_count,
           e0, mats, own_h, mask_h, cour_h, stok_h, oc,
           e_out, obuf1, drift, sea,
           ebuf, xbuf, low, elow, mbuf, stok, cour, ownv, maskv, obuf0,
           o0, o1, ux, uy, acc,
           epack, ehx, ehy, opack, ohx, ohy,
           lsem, esem, ersem, osem, orsem):
    g = lax.axis_index("grp")
    t = lax.axis_index("tile")
    ng = lax.axis_size("grp")
    nt = lax.axis_size("tile")
    bins = tiles * LANES
    points = rows * cols
    has = [g > 0, g < ng - 1, t > 0, t < nt - 1]
    peer = [{"grp": g - 1}, {"grp": g + 1}, {"tile": t - 1}, {"tile": t + 1}]
    back = [E, W, S, N]
    chunks = [(k, min(2, tiles - k)) for k in range(0, tiles, 2)]
    obuf = (obuf0, obuf1)
    fields = obuf0.shape[0]

    def place(m, k):
        full = tiles // 2
        return (m * (full + 1) + k // 2, k % 2) if k < 2 * full else (full, m)

    e4 = ebuf.reshape(tiles, rows + 2, PITCH, LANES)
    o4 = [o.reshape(fields, rows + 2, PITCH, LANES) for o in obuf]

    barrier = pltpu.get_barrier_semaphore()
    for d in range(4):
        @pl.when(has[d])
        def _(d=d):
            pl.semaphore_signal(barrier, inc=1, device_id=peer[d], device_id_type=pl.DeviceIdType.MESH)

    loads = []

    def load(src, dst):
        copy = pltpu.make_async_copy(src, dst, lsem.at[len(loads)])
        copy.start()
        loads.append(copy)
        return copy

    e_load = [load(e0.at[:, :, pl.ds(k * LANES, LANES)], e4.at[k, pl.ds(1, rows), pl.ds(LEAD, cols), :]) for k in range(tiles)]
    small = [load(oc, o4[0].at[:, pl.ds(1, rows), pl.ds(LEAD, cols), :]),
             load(cour_h, cour), load(mask_h, maskv), load(own_h, ownv)]
    for d in range(4):
        @pl.when(jnp.logical_not(has[d]))
        def _(d=d):
            if d < 2:
                ehx[:, d] = jnp.zeros_like(ehx[:, d])
                ohx[:, d] = jnp.zeros_like(ohx[:, d])
            else:
                ehy[:, d - 2] = jnp.zeros_like(ehy[:, d - 2])
                ohy[:, d - 2] = jnp.zeros_like(ohy[:, d - 2])

    def e_copy(step, d, c):
        k, width = chunks[c]
        span = pl.ds(k, width)
        far = back[d]
        if d < 2:
            src = epack.at[step, d, span]
            dst = ehx.at[step, far, span]
        else:
            src = e4.at[span, 1 if d == N else rows, pl.ds(LEAD, cols), :]
            dst = ehy.at[step, far - 2, span]
        return pltpu.make_async_remote_copy(
            src_ref=src, dst_ref=dst, send_sem=esem.at[step, d, c], recv_sem=ersem.at[step, far, c],
            device_id=peer[d], device_id_type=pl.DeviceIdType.MESH)

    def e_arrival(step, side, c):
        k, width = chunks[c]
        span = pl.ds(k, width)
        dst = ehx.at[step, side, span] if side < 2 else ehy.at[step, side - 2, span]
        return pltpu.make_async_remote_copy(
            src_ref=dst, dst_ref=dst, send_sem=esem.at[step, side, c], recv_sem=ersem.at[step, side, c],
            device_id=peer[side], device_id_type=pl.DeviceIdType.MESH)

    def o_copy(step, d):
        far = back[d]
        if d < 2:
            src = opack.at[step, d]
            dst = ohx.at[step, far]
        else:
            src = o4[step].at[:, 1 if d == N else rows, pl.ds(LEAD, cols), :]
            dst = ohy.at[step, far - 2]
        return pltpu.make_async_remote_copy(
            src_ref=src, dst_ref=dst, send_sem=osem.at[step, d], recv_sem=orsem.at[step, far],
            device_id=peer[d], device_id_type=pl.DeviceIdType.MESH)

    def o_arrival(step, side):
        dst = ohx.at[step, side] if side < 2 else ohy.at[step, side - 2]
        return pltpu.make_async_remote_copy(
            src_ref=dst, dst_ref=dst, send_sem=osem.at[step, side], recv_sem=orsem.at[step, side],
            device_id=peer[side], device_id_type=pl.DeviceIdType.MESH)

    first_col = pl.ds(PITCH + LEAD, rows, stride=PITCH)
    last_col = pl.ds(PITCH + LEAD + cols - 1, rows, stride=PITCH)
    west_col = pl.ds(PITCH + LEAD - 1, rows, stride=PITCH)
    east_col = pl.ds(PITCH + LEAD + cols, rows, stride=PITCH)

    def e_pack(step, c):
        k0, width = chunks[c]
        for k in range(k0, k0 + width):
            epack[step, W, k] = ebuf[k, first_col, :]
            epack[step, E, k] = ebuf[k, last_col, :]

    def o_pack(step):
        for q in range(fields):
            opack[step, W, q] = obuf[step][q, first_col, :]
            opack[step, E, q] = obuf[step][q, last_col, :]

    def send(make):
        for d in (N, S, W, E):
            @pl.when(has[d])
            def _(d=d):
                make(d).start()

    def wait_recv(make):
        for d in range(4):
            @pl.when(has[d])
            def _(d=d):
                make(d).wait_recv()

    def wait_send(make):
        for d in range(4):
            @pl.when(has[d])
            def _(d=d):
                make(d).wait_send()

    for c, (k0, width) in enumerate(chunks):
        for k in range(k0, k0 + width):
            e_load[k].wait()
        e_pack(0, c)
    m_load = []
    for m in range(mats_count):
        for k in range(0, tiles, 2):
            width = min(2, tiles - k)
            pair, half = place(m, k)
            m_load.append(load(mats.at[m, :, pl.ds(k * LANES, width * LANES)],
                               mbuf.at[pair, :, pl.ds(half * LANES, width * LANES)]))
    stok_load = load(stok_h, stok)
    pl.semaphore_wait(barrier, sum(h.astype(jnp.int32) for h in has))
    for c in range(len(chunks)):
        send(lambda d: e_copy(0, d, c))
    for copy in small:
        copy.wait()
    o_pack(0)
    send(lambda d: o_copy(0, d))

    mask_all = maskv[...].astype(jnp.float32)
    own_all = ownv[...]
    own0 = jnp.where(own_all == 0, 1.0, 0.0)
    own1 = jnp.where(own_all == 1, 1.0, 0.0)
    for r in range(rows):
        at = pl.ds(r * cols, cols)
        sea[at, :] = jnp.broadcast_to(mask_all[:, r:r + 1], (cols, LANES))
        o0[at, :] = jnp.broadcast_to(own0[:, r:r + 1], (cols, LANES))
        o1[at, :] = jnp.broadcast_to(own1[:, r:r + 1], (cols, LANES))

    def currents(slot):
        for r in range(rows):
            for q, dst in ((0, ux), (1, uy)):
                here = obuf[slot][q, pl.ds((r + 1) * PITCH + LEAD, cols), :]
                dst[r * cols:(r + 1) * cols, :] = current_gain * jnp.broadcast_to(here[:, 0:1], (cols, LANES))

    currents(0)

    def advect(k, base, at, stride=None):
        count = cols if stride is None else rows

        def near(shift):
            return ebuf[k, pl.ds(base + shift, count, stride=None if stride is None else PITCH), :]

        cx = jnp.broadcast_to(cour[0:1, k * LANES:(k + 1) * LANES], (count, LANES))
        cy = jnp.broadcast_to(cour[1:2, k * LANES:(k + 1) * LANES], (count, LANES))
        mid = near(0)
        sx = cx + ux[at, :]
        sy = cy + uy[at, :]
        flux = sx * jnp.where(sx > 0.0, mid - near(-1), near(1) - mid)
        flux = flux + sy * jnp.where(sy > 0.0, mid - near(-PITCH), near(PITCH) - mid)
        xbuf[k, at, :] = sea[at, :] * (mid - flux)

    def advect_all(k):
        @pl.loop(0, rows // 8)
        def _(block):
            for i in range(8):
                r = block * 8 + i
                advect(k, (r + 1) * PITCH + LEAD, pl.ds(pl.multiple_of(r * cols, cols), cols))

    def advect_border(k):
        for r in (0, rows - 1):
            advect(k, (r + 1) * PITCH + LEAD, pl.ds(r * cols, cols))
        for c in (0, cols - 1):
            advect(k, PITCH + LEAD + c, pl.ds(c, rows, stride=cols), cols)

    def lower(k):
        @pl.loop(0, rows // 8)
        def _(block):
            for i in range(8):
                at = pl.ds(pl.multiple_of((block * 8 + i) * cols, cols), cols)
                adv = xbuf[k, at, :]
                for m, chosen in ((0, o0), (1, o1)):
                    pair, half = place(m, k)
                    low[pair, at, half * LANES:(half + 1) * LANES] = (adv * chosen[at, :]).astype(jnp.bfloat16)

    def gather(c, first_tile):
        pairs = sorted({place(m, first_tile)[0] for m in range(mats_count)})
        for k0, width in chunks:
            src = 0.0
            for pair in pairs:
                src = src + lax.dot_general(
                    low[pair], mbuf[pair, k0 * LANES:(k0 + width) * LANES, :], (((1,), (1,)), ((), ())),
                    preferred_element_type=jnp.float32)
            for k in range(k0, k0 + width):
                part = src[:, (k - k0) * LANES:(k - k0 + 1) * LANES]
                if c > 0:
                    part = part + acc[k]
                if c + 1 < len(chunks):
                    acc[k] = part
                else:
                    new = sea[...] * (xbuf[k] + source_gain * part)
                    e_out[:, :, k * LANES:(k + 1) * LANES] = new.reshape(rows, cols, LANES)
                    elow[:, k * LANES:(k + 1) * LANES] = new.astype(jnp.bfloat16)

    def put(q, base, new):
        obuf[1][q, pl.ds(base, cols), :] = new

    for step in range(STEPS):
        for k in range(tiles):
            advect_all(k)
        for c, (k0, width) in enumerate(chunks):
            wait_recv(lambda d: e_arrival(step, d, c))
            for k in range(k0, k0 + width):
                ebuf[k, west_col, :] = ehx[step, W, k]
                ebuf[k, east_col, :] = ehx[step, E, k]
                ebuf[k, pl.ds(LEAD, cols), :] = ehy[step, 0, k]
                ebuf[k, pl.ds((rows + 1) * PITCH + LEAD, cols), :] = ehy[step, 1, k]
                advect_border(k)
                lower(k)
            if step + 1 == STEPS:
                gather(c, k0)
        for c in range(len(chunks)):
            wait_send(lambda d: e_copy(step, d, c))
        for c, (k0, width) in enumerate(chunks if step + 1 < STEPS else []):
            if step == 0 and c == 0:
                for copy in m_load:
                    copy.wait()
            src = 0.0
            for pair in range(tiles):
                src = src + lax.dot_general(
                    low[pair], mbuf[pair, k0 * LANES:(k0 + width) * LANES, :], (((1,), (1,)), ((), ())),
                    preferred_element_type=jnp.float32)
            for k in range(k0, k0 + width):
                part = src[:, (k - k0) * LANES:(k - k0 + 1) * LANES]
                new = sea[...] * (xbuf[k] + source_gain * part)
                e4[k, 1:rows + 1, LEAD:LEAD + cols, :] = new.reshape(rows, cols, LANES)
                elow[:, k * LANES:(k + 1) * LANES] = new.astype(jnp.bfloat16)
            if step + 1 < STEPS:
                e_pack(step + 1, c)
                send(lambda d: e_copy(step + 1, d, c))
        if step == 0:
            stok_load.wait()
        drift[...] = jnp.dot(elow[...], stok[...], preferred_element_type=jnp.float32)
        wait_recv(lambda d: o_arrival(step, d))
        for q in range(fields):
            obuf[step][q, west_col, :] = ohx[step, W, q]
            obuf[step][q, east_col, :] = ohx[step, E, q]
            obuf[step][q, pl.ds(LEAD, cols), :] = ohy[step, 0, q]
            obuf[step][q, pl.ds((rows + 1) * PITCH + LEAD, cols), :] = ohy[step, 1, q]
        if step == 1:
            wait_send(lambda d: o_copy(0, d))
        if step + 1 < STEPS:
            ocean_rows(obuf[0], drift, sea, 0, rows, cols, lambda q, r, at, base, new: put(q, base, new))
            currents(1 - step)
            o_pack(step + 1)
            send(lambda d: o_copy(step + 1, d))
    wait_send(lambda d: o_copy(1, d))


def local(spectrum, matrices, ownership, land_mask, courant, stokes_weight, ocean):
    bins, rows, cols = spectrum.shape
    mats = matrices.reshape(matrices.shape[2:])
    count = mats.shape[0]
    tiles = bins // LANES
    points = rows * cols
    fields = ocean.shape[0]
    chunk_count = -(-tiles // 2)
    flat = (rows + 2) * PITCH
    e0 = jnp.transpose(spectrum, (1, 2, 0))
    f32 = jnp.float32
    any_spec = pl.BlockSpec(memory_space=pltpu.HBM)
    e_new, o_mid, drift, sea = pl.pallas_call(
        functools.partial(kernel, rows, cols, tiles, count),
        out_shape=(jax.ShapeDtypeStruct((rows, cols, bins), f32), jax.ShapeDtypeStruct((fields, flat, LANES), f32),
                   jax.ShapeDtypeStruct((points, 2 * LANES), f32), jax.ShapeDtypeStruct((points, LANES), f32)),
        in_specs=[any_spec] * 7,
        out_specs=(pl.BlockSpec(memory_space=pltpu.VMEM),) * 4,
        scratch_shapes=[
            pltpu.VMEM((tiles, flat, LANES), f32),
            pltpu.VMEM((tiles, points, LANES), f32),
            pltpu.VMEM((tiles, points, 2 * LANES), jnp.bfloat16),
            pltpu.VMEM((points, bins), jnp.bfloat16),
            pltpu.VMEM((tiles, bins, 2 * LANES), jnp.bfloat16),
            pltpu.VMEM((bins, 2 * LANES), jnp.bfloat16),
            pltpu.VMEM((2, bins), f32),
            pltpu.VMEM((cols, rows), jnp.int32),
            pltpu.VMEM((cols, rows), jnp.int32),
            pltpu.VMEM((fields, flat, LANES), f32),
        ] + [pltpu.VMEM((points, LANES), f32)] * 4 + [
            pltpu.VMEM((tiles, points, LANES), f32),
            pltpu.VMEM((STEPS, 2, tiles, rows, LANES), f32),
            pltpu.VMEM((STEPS, 2, tiles, rows, LANES), f32),
            pltpu.VMEM((STEPS, 2, tiles, cols, LANES), f32),
            pltpu.VMEM((STEPS, 2, fields, rows, LANES), f32),
            pltpu.VMEM((STEPS, 2, fields, rows, LANES), f32),
            pltpu.VMEM((STEPS, 2, fields, cols, LANES), f32),
            pltpu.SemaphoreType.DMA((tiles + 5 + chunk_count * count,)),
            pltpu.SemaphoreType.DMA((STEPS, 4, chunk_count)),
            pltpu.SemaphoreType.DMA((STEPS, 4, chunk_count)),
            pltpu.SemaphoreType.DMA((STEPS, 4)),
            pltpu.SemaphoreType.DMA((STEPS, 4)),
        ],
        compiler_params=pltpu.CompilerParams(
            collective_id=0, has_side_effects=True, vmem_limit_bytes=34 * 1024 * 1024),
    )(*[pltpu.with_memory_space_constraint(x, pltpu.HBM) for x in (e0, mats, ownership.T, land_mask.T, courant, stokes_weight, ocean)])
    e_out, o_new = pl.pallas_call(
        functools.partial(last_kernel, rows, cols),
        out_shape=(jax.ShapeDtypeStruct((rows, cols, bins), f32), jax.ShapeDtypeStruct(ocean.shape, f32)),
        in_specs=[pl.BlockSpec(memory_space=pltpu.VMEM)] * 4,
        out_specs=(any_spec, any_spec),
        scratch_shapes=[pltpu.VMEM(ocean.shape, f32), pltpu.SemaphoreType.DMA((8,))],
        compiler_params=pltpu.CompilerParams(vmem_limit_bytes=16 * 1024 * 1024),
    )(e_new, o_mid, drift, sea)
    return jnp.transpose(e_out, (2, 0, 1)), o_new


def solution(mesh):
    in_specs = (
        P(None, "tile", "grp"),
        P("tile", "grp", None, None, None),
        P("tile", "grp"),
        P("tile", "grp"),
        P(),
        P(),
        P(None, "tile", "grp", None),
    )
    out_specs = (P(None, "tile", "grp"), P(None, "tile", "grp", None))
    return jax.shard_map(local, mesh=mesh, in_specs=in_specs, out_specs=out_specs, check_vma=False)
```

```python
import functools
import jax
import jax.numpy as jnp
from jax import lax
from jax.sharding import PartitionSpec as P
from jax.experimental import pallas as pl
from jax.experimental.pallas import tpu as pltpu

STEPS = 2
current_gain = 0.2
source_gain = 0.5
mixing_side = 0.15
mixing_depth = 0.2
rotation = 0.3
transport = 0.5

LANES = 128
PITCH = 24
LEAD = 8
OCEAN_UNROLL = 4
W, E, N, S = range(4)


def ocean_rows(obuf, drift, sea, first, last, cols, put):
    fields = obuf.shape[0]
    lane = lax.broadcasted_iota(jnp.int32, (cols, LANES), 1)

    @pl.loop(first, last, unroll=OCEAN_UNROLL)
    def _(r):
        base = (r + 1) * PITCH + LEAD
        at = pl.ds(pl.multiple_of(r * cols, cols), cols)
        d0 = drift[at, 0:LANES]
        d1 = drift[at, LANES:2 * LANES]
        sm = sea[at, :]
        mids = [obuf[q, pl.ds(base, cols), :] for q in range(fields)]
        for q in range(fields):
            mid = mids[q]
            west = obuf[q, pl.ds(base - 1, cols), :]
            east = obuf[q, pl.ds(base + 1, cols), :]
            north = obuf[q, pl.ds(base - PITCH, cols), :]
            south = obuf[q, pl.ds(base + PITCH, cols), :]
            above = jnp.where(lane == LANES - 1, 0.0, pltpu.roll(mid, LANES - 1, 1))
            below = jnp.where(lane == 0, 0.0, pltpu.roll(mid, 1, 1))
            mix = mixing_side * (north + south + west + east - 4.0 * mid) + mixing_depth * (above + below - 2.0 * mid)
            if q == 0:
                tend = mix + rotation * (mids[1] + d1)
            elif q == 1:
                tend = mix - rotation * (mids[0] + d0)
            else:
                tend = mix - transport * (d0 * (0.5 * (east - west)) + d1 * (0.5 * (south - north)))
            put(q, r, at, base, mid + sm * tend)


def last_kernel(rows, cols, e_new, obuf, drift, sea, e_out, o_out, stage, sem):
    copies = []
    blocks = 4
    size = rows // blocks

    def out(src, dst):
        copy = pltpu.make_async_copy(src, dst, sem.at[len(copies)])
        copy.start()
        copies.append(copy)

    def put(q, r, at, base, new):
        stage[q, r] = new

    for i in range(blocks):
        span = pl.ds(i * size, size)
        out(e_new.at[span], e_out.at[span])
    for i in range(blocks):
        span = pl.ds(i * size, size)
        ocean_rows(obuf, drift, sea, i * size, (i + 1) * size, cols, put)
        out(stage.at[:, span], o_out.at[:, span])
    for copy in copies:
        copy.wait()


def kernel(rows, cols, tiles, mats_count,
           e0, mats, own_h, mask_h, cour_h, stok_h, oc,
           e_out, obuf1, drift, sea,
           ebuf, xbuf, low, elow, mbuf, stok, cour, ownv, maskv, obuf0,
           o0, o1, ux, uy,
           epack, ehx, ehy, opack, ohx, ohy,
           lsem, esem, ersem, osem, orsem):
    g = lax.axis_index("grp")
    t = lax.axis_index("tile")
    ng = lax.axis_size("grp")
    nt = lax.axis_size("tile")
    bins = tiles * LANES
    points = rows * cols
    has = [g > 0, g < ng - 1, t > 0, t < nt - 1]
    peer = [{"grp": g - 1}, {"grp": g + 1}, {"tile": t - 1}, {"tile": t + 1}]
    back = [E, W, S, N]
    chunks = [(k, min(2, tiles - k)) for k in range(0, tiles, 2)]
    obuf = (obuf0, obuf1)
    fields = obuf0.shape[0]

    def place(m, k):
        full = tiles // 2
        return (m * (full + 1) + k // 2, k % 2) if k < 2 * full else (full, m)

    e4 = ebuf.reshape(tiles, rows + 2, PITCH, LANES)
    o4 = [o.reshape(fields, rows + 2, PITCH, LANES) for o in obuf]

    barrier = pltpu.get_barrier_semaphore()
    for d in range(4):
        @pl.when(has[d])
        def _(d=d):
            pl.semaphore_signal(barrier, inc=1, device_id=peer[d], device_id_type=pl.DeviceIdType.MESH)

    loads = []

    def load(src, dst):
        copy = pltpu.make_async_copy(src, dst, lsem.at[len(loads)])
        copy.start()
        loads.append(copy)
        return copy

    e_load = [load(e0.at[:, :, pl.ds(k * LANES, LANES)], e4.at[k, pl.ds(1, rows), pl.ds(LEAD, cols), :]) for k in range(tiles)]
    small = [load(oc, o4[0].at[:, pl.ds(1, rows), pl.ds(LEAD, cols), :]),
             load(cour_h, cour), load(mask_h, maskv), load(own_h, ownv)]
    for d in range(4):
        @pl.when(jnp.logical_not(has[d]))
        def _(d=d):
            if d < 2:
                ehx[:, d] = jnp.zeros_like(ehx[:, d])
                ohx[:, d] = jnp.zeros_like(ohx[:, d])
            else:
                ehy[:, d - 2] = jnp.zeros_like(ehy[:, d - 2])
                ohy[:, d - 2] = jnp.zeros_like(ohy[:, d - 2])

    def e_copy(step, d, c):
        k, width = chunks[c] if step else (0, tiles)
        span = pl.ds(k, width)
        far = back[d]
        if d < 2:
            src = epack.at[step, d, span]
            dst = ehx.at[step, far, span]
        else:
            src = e4.at[span, 1 if d == N else rows, pl.ds(LEAD, cols), :]
            dst = ehy.at[step, far - 2, span]
        return pltpu.make_async_remote_copy(
            src_ref=src, dst_ref=dst, send_sem=esem.at[step, d, c], recv_sem=ersem.at[step, far, c],
            device_id=peer[d], device_id_type=pl.DeviceIdType.MESH)

    def e_arrival(step, side, c):
        k, width = chunks[c] if step else (0, tiles)
        span = pl.ds(k, width)
        dst = ehx.at[step, side, span] if side < 2 else ehy.at[step, side - 2, span]
        return pltpu.make_async_remote_copy(
            src_ref=dst, dst_ref=dst, send_sem=esem.at[step, side, c], recv_sem=ersem.at[step, side, c],
            device_id=peer[side], device_id_type=pl.DeviceIdType.MESH)

    def o_copy(step, d):
        far = back[d]
        if d < 2:
            src = opack.at[step, d]
            dst = ohx.at[step, far]
        else:
            src = o4[step].at[:, 1 if d == N else rows, pl.ds(LEAD, cols), :]
            dst = ohy.at[step, far - 2]
        return pltpu.make_async_remote_copy(
            src_ref=src, dst_ref=dst, send_sem=osem.at[step, d], recv_sem=orsem.at[step, far],
            device_id=peer[d], device_id_type=pl.DeviceIdType.MESH)

    def o_arrival(step, side):
        dst = ohx.at[step, side] if side < 2 else ohy.at[step, side - 2]
        return pltpu.make_async_remote_copy(
            src_ref=dst, dst_ref=dst, send_sem=osem.at[step, side], recv_sem=orsem.at[step, side],
            device_id=peer[side], device_id_type=pl.DeviceIdType.MESH)

    first_col = pl.ds(PITCH + LEAD, rows, stride=PITCH)
    last_col = pl.ds(PITCH + LEAD + cols - 1, rows, stride=PITCH)
    west_col = pl.ds(PITCH + LEAD - 1, rows, stride=PITCH)
    east_col = pl.ds(PITCH + LEAD + cols, rows, stride=PITCH)

    def e_pack(step, c):
        k0, width = chunks[c]
        for k in range(k0, k0 + width):
            epack[step, W, k] = ebuf[k, first_col, :]
            epack[step, E, k] = ebuf[k, last_col, :]

    def o_pack(step):
        for q in range(fields):
            opack[step, W, q] = obuf[step][q, first_col, :]
            opack[step, E, q] = obuf[step][q, last_col, :]

    def send(make):
        for d in (N, S, W, E):
            @pl.when(has[d])
            def _(d=d):
                make(d).start()

    def wait_recv(make):
        for d in range(4):
            @pl.when(has[d])
            def _(d=d):
                make(d).wait_recv()

    def wait_send(make):
        for d in range(4):
            @pl.when(has[d])
            def _(d=d):
                make(d).wait_send()

    for c, (k0, width) in enumerate(chunks):
        for k in range(k0, k0 + width):
            e_load[k].wait()
        e_pack(0, c)
    m_load = []
    for m in range(mats_count):
        for k in range(0, tiles, 2):
            width = min(2, tiles - k)
            pair, half = place(m, k)
            m_load.append(load(mats.at[m, :, pl.ds(k * LANES, width * LANES)],
                               mbuf.at[pair, :, pl.ds(half * LANES, width * LANES)]))
    stok_load = load(stok_h, stok)
    pl.semaphore_wait(barrier, sum(h.astype(jnp.int32) for h in has))
    send(lambda d: e_copy(0, d, 0))
    for copy in small:
        copy.wait()
    o_pack(0)
    send(lambda d: o_copy(0, d))

    mask_all = maskv[...].astype(jnp.float32)
    own_all = ownv[...]
    own0 = jnp.where(own_all == 0, 1.0, 0.0)
    own1 = jnp.where(own_all == 1, 1.0, 0.0)
    for r in range(rows):
        at = pl.ds(r * cols, cols)
        sea[at, :] = jnp.broadcast_to(mask_all[:, r:r + 1], (cols, LANES))
        o0[at, :] = jnp.broadcast_to(own0[:, r:r + 1], (cols, LANES))
        o1[at, :] = jnp.broadcast_to(own1[:, r:r + 1], (cols, LANES))

    def currents(slot):
        for r in range(rows):
            for q, dst in ((0, ux), (1, uy)):
                here = obuf[slot][q, pl.ds((r + 1) * PITCH + LEAD, cols), :]
                dst[r * cols:(r + 1) * cols, :] = current_gain * jnp.broadcast_to(here[:, 0:1], (cols, LANES))

    currents(0)

    def advect(k, base, at, stride=None):
        count = cols if stride is None else rows

        def near(shift):
            return ebuf[k, pl.ds(base + shift, count, stride=None if stride is None else PITCH), :]

        cx = jnp.broadcast_to(cour[0:1, k * LANES:(k + 1) * LANES], (count, LANES))
        cy = jnp.broadcast_to(cour[1:2, k * LANES:(k + 1) * LANES], (count, LANES))
        mid = near(0)
        sx = cx + ux[at, :]
        sy = cy + uy[at, :]
        flux = sx * jnp.where(sx > 0.0, mid - near(-1), near(1) - mid)
        flux = flux + sy * jnp.where(sy > 0.0, mid - near(-PITCH), near(PITCH) - mid)
        xbuf[k, at, :] = sea[at, :] * (mid - flux)

    def advect_all(k):
        @pl.loop(0, rows // 8)
        def _(block):
            for i in range(8):
                r = block * 8 + i
                advect(k, (r + 1) * PITCH + LEAD, pl.ds(pl.multiple_of(r * cols, cols), cols))

    def advect_border(k):
        for r in (0, rows - 1):
            advect(k, (r + 1) * PITCH + LEAD, pl.ds(r * cols, cols))
        for c in (0, cols - 1):
            advect(k, PITCH + LEAD + c, pl.ds(c, rows, stride=cols), cols)

    def lower(k):
        @pl.loop(0, rows // 8)
        def _(block):
            for i in range(8):
                at = pl.ds(pl.multiple_of((block * 8 + i) * cols, cols), cols)
                adv = xbuf[k, at, :]
                for m, chosen in ((0, o0), (1, o1)):
                    pair, half = place(m, k)
                    low[pair, at, half * LANES:(half + 1) * LANES] = (adv * chosen[at, :]).astype(jnp.bfloat16)

    def put(q, base, new):
        obuf[1][q, pl.ds(base, cols), :] = new

    for step in range(STEPS):
        for k in range(tiles):
            advect_all(k)
        for c, (k0, width) in enumerate(chunks):
            if step or c == 0:
                wait_recv(lambda d: e_arrival(step, d, c))
            for k in range(k0, k0 + width):
                ebuf[k, west_col, :] = ehx[step, W, k]
                ebuf[k, east_col, :] = ehx[step, E, k]
                ebuf[k, pl.ds(LEAD, cols), :] = ehy[step, 0, k]
                ebuf[k, pl.ds((rows + 1) * PITCH + LEAD, cols), :] = ehy[step, 1, k]
                advect_border(k)
                lower(k)
        for c in range(len(chunks) if step else 1):
            wait_send(lambda d: e_copy(step, d, c))
        for c, (k0, width) in enumerate(chunks):
            if step == 0 and c == 0:
                for copy in m_load:
                    copy.wait()
            src = 0.0
            for pair in range(tiles):
                src = src + lax.dot_general(
                    low[pair], mbuf[pair, k0 * LANES:(k0 + width) * LANES, :], (((1,), (1,)), ((), ())),
                    preferred_element_type=jnp.float32)
            for k in range(k0, k0 + width):
                part = src[:, (k - k0) * LANES:(k - k0 + 1) * LANES]
                new = sea[...] * (xbuf[k] + source_gain * part)
                if step + 1 < STEPS:
                    e4[k, 1:rows + 1, LEAD:LEAD + cols, :] = new.reshape(rows, cols, LANES)
                else:
                    e_out[:, :, k * LANES:(k + 1) * LANES] = new.reshape(rows, cols, LANES)
                elow[:, k * LANES:(k + 1) * LANES] = new.astype(jnp.bfloat16)
            if step + 1 < STEPS:
                e_pack(step + 1, c)
                send(lambda d: e_copy(step + 1, d, c))
        if step == 0:
            stok_load.wait()
        drift[...] = jnp.dot(elow[...], stok[...], preferred_element_type=jnp.float32)
        wait_recv(lambda d: o_arrival(step, d))
        for q in range(fields):
            obuf[step][q, west_col, :] = ohx[step, W, q]
            obuf[step][q, east_col, :] = ohx[step, E, q]
            obuf[step][q, pl.ds(LEAD, cols), :] = ohy[step, 0, q]
            obuf[step][q, pl.ds((rows + 1) * PITCH + LEAD, cols), :] = ohy[step, 1, q]
        if step == 1:
            wait_send(lambda d: o_copy(0, d))
        if step + 1 < STEPS:
            ocean_rows(obuf[0], drift, sea, 0, rows, cols, lambda q, r, at, base, new: put(q, base, new))
            currents(1 - step)
            o_pack(step + 1)
            send(lambda d: o_copy(step + 1, d))
    wait_send(lambda d: o_copy(1, d))


def local(spectrum, matrices, ownership, land_mask, courant, stokes_weight, ocean):
    bins, rows, cols = spectrum.shape
    mats = matrices.reshape(matrices.shape[2:])
    count = mats.shape[0]
    tiles = bins // LANES
    points = rows * cols
    fields = ocean.shape[0]
    chunk_count = -(-tiles // 2)
    flat = (rows + 2) * PITCH
    e0 = jnp.transpose(spectrum, (1, 2, 0))
    f32 = jnp.float32
    any_spec = pl.BlockSpec(memory_space=pltpu.HBM)
    e_new, o_mid, drift, sea = pl.pallas_call(
        functools.partial(kernel, rows, cols, tiles, count),
        out_shape=(jax.ShapeDtypeStruct((rows, cols, bins), f32), jax.ShapeDtypeStruct((fields, flat, LANES), f32),
                   jax.ShapeDtypeStruct((points, 2 * LANES), f32), jax.ShapeDtypeStruct((points, LANES), f32)),
        in_specs=[any_spec] * 7,
        out_specs=(pl.BlockSpec(memory_space=pltpu.VMEM),) * 4,
        scratch_shapes=[
            pltpu.VMEM((tiles, flat, LANES), f32),
            pltpu.VMEM((tiles, points, LANES), f32),
            pltpu.VMEM((tiles, points, 2 * LANES), jnp.bfloat16),
            pltpu.VMEM((points, bins), jnp.bfloat16),
            pltpu.VMEM((tiles, bins, 2 * LANES), jnp.bfloat16),
            pltpu.VMEM((bins, 2 * LANES), jnp.bfloat16),
            pltpu.VMEM((2, bins), f32),
            pltpu.VMEM((cols, rows), jnp.int32),
            pltpu.VMEM((cols, rows), jnp.int32),
            pltpu.VMEM((fields, flat, LANES), f32),
        ] + [pltpu.VMEM((points, LANES), f32)] * 4 + [
            pltpu.VMEM((STEPS, 2, tiles, rows, LANES), f32),
            pltpu.VMEM((STEPS, 2, tiles, rows, LANES), f32),
            pltpu.VMEM((STEPS, 2, tiles, cols, LANES), f32),
            pltpu.VMEM((STEPS, 2, fields, rows, LANES), f32),
            pltpu.VMEM((STEPS, 2, fields, rows, LANES), f32),
            pltpu.VMEM((STEPS, 2, fields, cols, LANES), f32),
            pltpu.SemaphoreType.DMA((tiles + 5 + chunk_count * count,)),
            pltpu.SemaphoreType.DMA((STEPS, 4, chunk_count)),
            pltpu.SemaphoreType.DMA((STEPS, 4, chunk_count)),
            pltpu.SemaphoreType.DMA((STEPS, 4)),
            pltpu.SemaphoreType.DMA((STEPS, 4)),
        ],
        compiler_params=pltpu.CompilerParams(
            collective_id=0, has_side_effects=True, vmem_limit_bytes=34 * 1024 * 1024),
    )(*[pltpu.with_memory_space_constraint(x, pltpu.HBM) for x in (e0, mats, ownership.T, land_mask.T, courant, stokes_weight, ocean)])
    e_out, o_new = pl.pallas_call(
        functools.partial(last_kernel, rows, cols),
        out_shape=(jax.ShapeDtypeStruct((rows, cols, bins), f32), jax.ShapeDtypeStruct(ocean.shape, f32)),
        in_specs=[pl.BlockSpec(memory_space=pltpu.VMEM)] * 4,
        out_specs=(any_spec, any_spec),
        scratch_shapes=[pltpu.VMEM(ocean.shape, f32), pltpu.SemaphoreType.DMA((8,))],
        compiler_params=pltpu.CompilerParams(vmem_limit_bytes=16 * 1024 * 1024),
    )(e_new, o_mid, drift, sea)
    return jnp.transpose(e_out, (2, 0, 1)), o_new


def solution(mesh):
    in_specs = (
        P(None, "tile", "grp"),
        P("tile", "grp", None, None, None),
        P("tile", "grp"),
        P("tile", "grp"),
        P(),
        P(),
        P(None, "tile", "grp", None),
    )
    out_specs = (P(None, "tile", "grp"), P(None, "tile", "grp", None))
    return jax.shard_map(local, mesh=mesh, in_specs=in_specs, out_specs=out_specs, check_vma=False)
```
